32 devices in a mesh: ez: 4 (over z), ey: 2 (over y), ex: 4 (over x, core).
Axes of the slice: x: 2, y: 2, z: 4, core: 2. Of those that a mesh axis runs over, the one named last changes fastest.
Arguments:
- tokens: bfloat16 [8192, 2048], P(('ez', 'ey', 'ex'))
- expert_ids: int32 [8192, 8], P(('ez', 'ey', 'ex'))
- gate_weights: float32 [8192, 8], P(('ez', 'ey', 'ex'))
- w_gate: bfloat16 [128, 2048, 768], P(('ez', 'ey', 'ex'))
- w_up: bfloat16 [128, 2048, 768], P(('ez', 'ey', 'ex'))
- w_down: bfloat16 [128, 768, 2048], P(('ez', 'ey', 'ex'))
Outputs:
- output: bfloat16 [8192, 2048], P(('ez', 'ey', 'ex'))
All inputs are finite; a program needn't handle non-finite values.
Results may differ from the reference program's by a relative error of at most 0.00586641.
Values are sent between devices in bfloat16 or wider.
A program may use at most 1 GiB of HBM per device.

```python
import jax
import jax.numpy as jnp
from jax import lax

HIDDEN = 2048
EXPERT_FF = 768
EXPERTS = 128
TOP_K = 8
TOKENS = 256
DEVICES = 32
TOTAL_TOK = DEVICES * TOKENS
LOCAL_EXPERTS = EXPERTS // DEVICES
PER_EXPERT = TOTAL_TOK * TOP_K // EXPERTS


def draw_routing(route_key):
    def one_source(src_key):
        key_first, key_rest, key_dev, key_order = jax.random.split(src_key, 4)
        first_block = jax.random.permutation(key_first, LOCAL_EXPERTS)
        rest_block = jax.random.permutation(key_rest, EXPERTS - LOCAL_EXPERTS) + LOCAL_EXPERTS
        positions = jnp.arange(EXPERTS)
        spaced = positions % DEVICES == 0
        first_idx = jnp.clip(positions // DEVICES, 0, LOCAL_EXPERTS - 1)
        rest_idx = jnp.clip(positions - positions // DEVICES - 1, 0, EXPERTS - LOCAL_EXPERTS - 1)
        expert_cycle = jnp.where(spaced, first_block[first_idx], rest_block[rest_idx])
        dev_perm = jax.random.permutation(key_dev, DEVICES)
        expert_cycle = dev_perm[expert_cycle // LOCAL_EXPERTS] * LOCAL_EXPERTS + expert_cycle % LOCAL_EXPERTS
        tok_perm = jax.random.permutation(key_order, TOKENS)
        slot_pos = tok_perm[:, None] * TOP_K + jnp.arange(TOP_K)[None, :]
        return expert_cycle[slot_pos % EXPERTS]
    src_keys = jax.random.split(route_key, DEVICES)
    return jax.vmap(one_source)(src_keys).reshape(TOTAL_TOK, TOP_K).astype(jnp.int32)


def setup_inputs(seed: int = 0) -> dict:
    root_key = jax.random.key(seed)
    key_tok, key_ids, key_gate, key_w1, key_w3, key_w2 = jax.random.split(root_key, 6)
    tokens = jax.random.normal(key_tok, (TOTAL_TOK, HIDDEN), jnp.float32).astype(jnp.bfloat16)
    expert_ids = draw_routing(key_ids)
    gate_logits = 0.7 * jax.random.normal(key_gate, (TOTAL_TOK, TOP_K), jnp.float32)
    gate_weights = jax.nn.softmax(gate_logits, axis=-1)
    w_gate = (jax.random.normal(key_w1, (EXPERTS, HIDDEN, EXPERT_FF), jnp.float32) * HIDDEN ** -0.5).astype(jnp.bfloat16)
    w_up = (jax.random.normal(key_w3, (EXPERTS, HIDDEN, EXPERT_FF), jnp.float32) * HIDDEN ** -0.5).astype(jnp.bfloat16)
    w_down = (jax.random.normal(key_w2, (EXPERTS, EXPERT_FF, HIDDEN), jnp.float32) * (2.0 * EXPERT_FF ** -0.5)).astype(jnp.bfloat16)
    return {"tokens": tokens, "expert_ids": expert_ids, "gate_weights": gate_weights, "w_gate": w_gate, "w_up": w_up, "w_down": w_down}


def reference(tokens, expert_ids, gate_weights, w_gate, w_up, w_down):
    sort_order = jnp.argsort(expert_ids.reshape(-1), stable=True)
    rows_by_expert = (sort_order // TOP_K).reshape(EXPERTS, PER_EXPERT)
    gates_by_expert = gate_weights.reshape(-1)[sort_order].reshape(EXPERTS, PER_EXPERT)

    def expert_step(acc_out, expert_args):
        row_ids, row_gates, gate_mat, up_mat, down_mat = expert_args
        x_rows = tokens[row_ids]
        gate_act = jnp.dot(x_rows, gate_mat, preferred_element_type=jnp.float32)
        up_act = jnp.dot(x_rows, up_mat, preferred_element_type=jnp.float32)
        hidden_act = (jax.nn.silu(gate_act) * up_act).astype(jnp.bfloat16)
        expert_out = jnp.dot(hidden_act, down_mat, preferred_element_type=jnp.float32)
        acc_out = acc_out.at[row_ids].add(expert_out * row_gates[:, None])
        return acc_out, None

    init_acc = jnp.zeros((TOTAL_TOK, HIDDEN), jnp.float32)
    moe_sum = lax.scan(expert_step, init_acc, (rows_by_expert, gates_by_expert, w_gate, w_up, w_down))[0]
    return (tokens.astype(jnp.float32) + moe_sum).astype(jnp.bfloat16)
```

```python
import functools
import math

import jax
import jax.numpy as jnp
from jax import lax
from jax.experimental import pallas as pl
from jax.experimental.pallas import tpu as pltpu
from jax.sharding import PartitionSpec as P

MESH = pl.DeviceIdType.MESH
F32 = jnp.float32
BF16 = jnp.bfloat16


def routing_tables(expert_ids, gate_weights, num_devices, local_experts, capacity):
    tok_dev = expert_ids.shape[0]
    dev_hit = jnp.any((expert_ids // local_experts)[:, :, None] == jnp.arange(num_devices)[None, None, :], axis=1)
    slot_pos = jnp.where(dev_hit, jnp.cumsum(dev_hit.astype(jnp.int32), axis=0) - 1, -1)
    all_experts = jnp.arange(num_devices * local_experts)
    gate_dense = jnp.sum(jnp.where(expert_ids[:, :, None] == all_experts[None, None, :], gate_weights[:, :, None], 0.0), axis=1)
    gate_dense = gate_dense.reshape(tok_dev, num_devices, local_experts)
    place = slot_pos[:, :, None] == jnp.arange(capacity)[None, None, :]
    slot_gates = jnp.sum(jnp.where(place[:, :, None, :], gate_dense[:, :, :, None], 0.0), axis=0)
    return slot_pos.T, slot_gates


def moe_kernel(
    dims, x_ref, slot_ref, sgate_ref, w1_ref, w3_ref, w2_ref, out_ref,
    xall, smap, grecv, place, sbuf, drecv, rrecv, zret, acc, hbuf, gb, wb1, wb3, wb2,
    x_sem, w_sem, zs_send, zs_recv, sm_send, sm_recv, g_send, g_recv, d_send, d_recv, r_send, r_recv, zr_send, zr_recv,
):
    nz, ny, nx = dims
    nq = ny * nx
    ndev = nz * nq
    tok, hid = xall.shape[1:]
    cap = sbuf.shape[2]
    ff = wb1.shape[2]
    rows = nq * cap
    nt = 256
    ft = 256
    z = lax.axis_index("ez")
    q = lax.axis_index("ey") * nx + lax.axis_index("ex")
    me = z * nq + q

    def at(zz, qq):
        return (zz, lax.div(qq, nx), lax.rem(qq, nx))

    def rcopy(src, dst, ss, rs, dev):
        return pltpu.make_async_remote_copy(src_ref=src, dst_ref=dst, send_sem=ss, recv_sem=rs, device_id=dev, device_id_type=MESH)

    inner = lax.div(z * (3 - z), 2)
    flip = lax.div(z, 2)

    def mirrored(b):
        return b + flip * (3 - 2 * b)

    k1, k2, k3 = mirrored(1 - inner), mirrored(2), mirrored(3)

    def plane_of(s):
        return (
            z * lax.div(3 - s, 3)
            + k1 * (lax.rem(s, 2) * lax.div(4 - s, 3))
            + k2 * ((1 - lax.rem(s, 2)) * lax.div(s, 2))
            + k3 * lax.div(s, 3)
        )

    def peer(o):
        return lax.rem(q + o, nq)

    def weight_copies(e, slot):
        return (
            pltpu.make_async_copy(w1_ref.at[e], wb1.at[slot], w_sem.at[slot, 0]),
            pltpu.make_async_copy(w3_ref.at[e], wb3.at[slot], w_sem.at[slot, 1]),
            pltpu.make_async_copy(w2_ref.at[e], wb2.at[slot], w_sem.at[slot, 2]),
        )

    def z_rows(k, dst_z, n):
        return rcopy(xall.at[k], xall.at[k], zs_send.at[n], zs_recv.at[k], at(dst_z, q))

    def z_wait(k):
        rcopy(xall.at[k], xall.at[k], zs_send.at[0], zs_recv.at[k], at(z, q)).wait_recv()
        rcopy(smap.at[k], smap.at[k], sm_send.at[0], sm_recv.at[k], at(z, q)).wait_recv()

    def slot_copy(o):
        dz = lax.rem(z + o, nz)
        return rcopy(slot_ref.at[dz], smap.at[z], sm_send.at[o], sm_recv.at[z], at(dz, q))

    def gate_copy(o):
        d = lax.rem(me + o, ndev)
        return rcopy(sgate_ref.at[d], grecv.at[me], g_send.at[o], g_recv.at[me], at(lax.div(d, nq), lax.rem(d, nq)))

    def d_copy(k, half, o):
        return rcopy(sbuf.at[half, peer(o)], drecv.at[k, q], d_send.at[half, o], d_recv.at[k, q], at(z, peer(o)))

    def r_copy(k, o):
        return rcopy(drecv.at[k, peer(o)], rrecv.at[k, q], r_send.at[k, o], r_recv.at[k, q], at(z, peer(o)))

    def zr_copy(k):
        return rcopy(xall.at[k], zret.at[z], zr_send.at[k], zr_recv.at[z], at(k, q))

    def pack_and_send(s):
        k = plane_of(s)
        half = s % 2
        if s >= 2:
            for o in range(1, nq):
                d_copy(plane_of(s - 2), half, o).wait_send()
        lane_slot = lax.broadcasted_iota(jnp.int32, (cap, tok), 0)
        for d in range(nq):
            hit = lane_slot == smap[k, d : d + 1, :]
            place[k, d * cap : (d + 1) * cap, :] = jnp.where(hit, 1.0, 0.0).astype(BF16)

        @pl.loop(0, hid // nt)
        def _(n):
            cols = pl.ds(pl.multiple_of(n * nt, nt), nt)
            got = jnp.dot(place[k], xall[k, :, cols], preferred_element_type=F32).astype(BF16)
            sbuf[half, :, :, cols] = got.reshape(nq, cap, nt)

        for o in range(1, nq):
            d_copy(k, half, o).start()

        @pl.loop(0, hid // nt)
        def _(n):
            cols = pl.ds(pl.multiple_of(n * nt, nt), nt)
            drecv[k, q, :, cols] = sbuf[half, q, :, cols]

    def d_wait(k):
        for o in range(1, nq):
            r = peer(o)
            rcopy(sbuf.at[0, 0], drecv.at[k, r], d_send.at[0, o], d_recv.at[k, r], at(z, q)).wait_recv()

    def send_back(k):
        for o in range(1, nq):
            r_copy(k, o).start()

        @pl.loop(0, hid // nt)
        def _(n):
            cols = pl.ds(pl.multiple_of(n * nt, nt), nt)
            rrecv[k, q, :, cols] = drecv[k, q, :, cols]

    def r_wait(k):
        for o in range(1, nq):
            r = peer(o)
            rcopy(sbuf.at[0, 0], rrecv.at[k, r], r_send.at[0, o], r_recv.at[k, r], at(z, q)).wait_recv()

    def summed(k, cols):
        got = rrecv[k, :, :, cols].reshape(rows, nt)
        return lax.dot_general(place[k], got, (((0,), (0,)), ((), ())), preferred_element_type=F32)

    def unpack_and_send(k):
        r_wait(k)

        @pl.loop(0, hid // nt)
        def _(n):
            cols = pl.ds(pl.multiple_of(n * nt, nt), nt)
            xall[k, :, cols] = summed(k, cols).astype(BF16)

        zr_copy(k).start()

    for c in weight_copies(0, 0):
        c.start()
    load_x = pltpu.make_async_copy(x_ref, xall.at[z], x_sem)
    load_x.start()
    for o in range(1, nz):
        slot_copy(o).start()
    load_x.wait()

    @pl.when(z > 0)
    def _():
        z_rows(z, z - 1, 0).start()

    @pl.when(z < nz - 1)
    def _():
        z_rows(z, z + 1, 1).start()

    for o in range(1, ndev):
        gate_copy(o).start()
    smap[z] = slot_ref[z]
    grecv[me] = sgate_ref[me]
    pack_and_send(0)

    z_wait(k1)

    @pl.when(inner == 1)
    def _():
        z_wait(k2)
        z_rows(k1, k2, 2).start()
        z_rows(k2, k1, 3).start()

    pack_and_send(1)
    for o in range(1, ndev):
        s = lax.rem(me + o, ndev)
        rcopy(sgate_ref.at[0], grecv.at[s], g_send.at[o], g_recv.at[s], at(z, q)).wait_recv()

    def expert_step(i, _):
        s, e, slot = lax.div(i, 4), lax.rem(i, 4), lax.rem(i, 2)
        k = plane_of(s)

        @pl.when(i < 15)
        def _():
            for c in weight_copies(lax.rem(i + 1, 4), 1 - slot):
                c.start()

        @pl.when(i == 3)
        def _():
            @pl.when(inner == 0)
            def _():
                z_wait(k2)

            @pl.when(inner == 1)
            def _():
                z_wait(k3)
                z_rows(k3, k1, 4).start()

            pack_and_send(2)

        @pl.when(i == 7)
        def _():
            @pl.when(inner == 0)
            def _():
                z_wait(k3)

            pack_and_send(3)

        @pl.when(i == 8)
        def _():
            send_back(k1)

        @pl.when(i == 12)
        def _():
            send_back(k2)

        @pl.when(i == 14)
        def _():
            @pl.when(inner == 1)
            def _():
                z_rows(k1, k2, 2).wait_send()
                z_rows(k2, k1, 3).wait_send()
                z_rows(k3, k1, 4).wait_send()

            unpack_and_send(k1)

        @pl.when(e == 0)
        def _():
            d_wait(k)
            by_slot = grecv[pl.ds(k * nq, nq)].reshape(nq * 8, 128).T
            for r in range(nq):
                for j in range(4):
                    col = by_slot[0:cap, r * 8 + j : r * 8 + j + 1]
                    gb[j, r * cap : (r + 1) * cap, :] = jnp.broadcast_to(col, (cap, 128))

        for c in weight_copies(e, slot):
            c.wait()

        @pl.loop(0, ff // ft)
        def _(n):
            cols = pl.ds(pl.multiple_of(n * ft, ft), ft)
            xin = drecv[k].reshape(rows, hid)
            a = jnp.dot(xin, wb1[slot, :, cols], preferred_element_type=F32)
            b = jnp.dot(xin, wb3[slot, :, cols], preferred_element_type=F32)
            hbuf[:, cols] = (a * jax.nn.sigmoid(a) * b).astype(BF16)

        @pl.loop(0, hid // nt)
        def _(n):
            cols = pl.ds(pl.multiple_of(n * nt, nt), nt)
            o = jnp.dot(hbuf[...], wb2[slot, :, cols], preferred_element_type=F32)
            g = jnp.concatenate([gb[e]] * (nt // 128), axis=1)
            term = jnp.where(g > 0.0, o * g, 0.0)
            acc[:, cols] = jnp.where(e == 0, 0.0, acc[:, cols]) + term

        @pl.when(e == 3)
        def _():
            @pl.loop(0, hid // nt)
            def _(n):
                cols = pl.ds(pl.multiple_of(n * nt, nt), nt)
                drecv[k, :, :, cols] = acc[:, cols].astype(BF16).reshape(nq, cap, nt)

        return 0

    lax.fori_loop(0, 16, expert_step, 0)
    send_back(k3)
    send_back(z)
    unpack_and_send(k2)
    unpack_and_send(k3)
    r_wait(z)
    for o in range(1, nz):
        k = lax.rem(z + o, nz)
        rcopy(xall.at[k], zret.at[k], zr_send.at[0], zr_recv.at[k], at(z, q)).wait_recv()

    @pl.loop(0, hid // nt)
    def _(n):
        cols = pl.ds(pl.multiple_of(n * nt, nt), nt)
        total = summed(z, cols) + xall[z, :, cols].astype(F32)
        for o in range(1, nz):
            total = total + zret[lax.rem(z + o, nz), :, cols].astype(F32)
        out_ref[:, cols] = total.astype(BF16)

    @pl.when(z > 0)
    def _():
        z_rows(z, z - 1, 0).wait_send()

    @pl.when(z < nz - 1)
    def _():
        z_rows(z, z + 1, 1).wait_send()

    for o in range(1, nz):
        slot_copy(o).wait_send()
        zr_copy(lax.rem(z + o, nz)).wait_send()
    for o in range(1, ndev):
        gate_copy(o).wait_send()
    for o in range(1, nq):
        d_copy(k2, 0, o).wait_send()
        d_copy(k3, 1, o).wait_send()
        for s in range(4):
            r_copy(plane_of(s), o).wait_send()


def moe_call(dims, x, slots, slot_gates, w1, w3, w2, capacity):
    nz, ny, nx = dims
    nq = ny * nx
    ndev = nz * nq
    tok, hid = x.shape
    ff = w1.shape[2]
    dma = pltpu.SemaphoreType.DMA
    vmem = pl.BlockSpec(memory_space=pltpu.VMEM)
    hbm = pl.BlockSpec(memory_space=pl.ANY)
    return pl.pallas_call(
        functools.partial(moe_kernel, dims),
        out_shape=jax.ShapeDtypeStruct((tok, hid), BF16),
        in_specs=[hbm, vmem, vmem, hbm, hbm, hbm],
        out_specs=vmem,
        scratch_shapes=[
            pltpu.VMEM((nz, tok, hid), BF16),
            pltpu.VMEM((nz, nq, tok), jnp.int32),
            pltpu.VMEM((ndev, 8, 128), F32),
            pltpu.VMEM((nz, nq * capacity, tok), BF16),
            pltpu.VMEM((2, nq, capacity, hid), BF16),
            pltpu.VMEM((nz, nq, capacity, hid), BF16),
            pltpu.VMEM((nz, nq, capacity, hid), BF16),
            pltpu.VMEM((nz, tok, hid), BF16),
            pltpu.VMEM((nq * capacity, hid), F32),
            pltpu.VMEM((nq * capacity, ff), BF16),
            pltpu.VMEM((4, nq * capacity, 128), F32),
            pltpu.VMEM((2, hid, ff), BF16),
            pltpu.VMEM((2, hid, ff), BF16),
            pltpu.VMEM((2, ff, hid), BF16),
            dma,
            dma((2, 3)),
            dma((5,)),
            dma((nz,)),
            dma((nz,)),
            dma((nz,)),
            dma((ndev,)),
            dma((ndev,)),
            dma((2, nq)),
            dma((nz, nq)),
            dma((nz, nq)),
            dma((nz, nq)),
            dma((nz,)),
            dma((nz,)),
        ],
        compiler_params=pltpu.CompilerParams(has_side_effects=True, vmem_limit_bytes=66 * 1000 * 1000),
    )(x, slots, slot_gates, w1, w3, w2)


def solution(mesh):
    ep_axes = tuple(mesh.axis_names)
    dims = tuple(mesh.shape[axis_name] for axis_name in ep_axes)
    num_devices = math.prod(dims)
    row_spec = P(ep_axes, None)
    w_spec = P(ep_axes, None, None)

    def local_layer(tokens, expert_ids, gate_weights, w_gate, w_up, w_down):
        tok_dev = tokens.shape[0]
        top_k = expert_ids.shape[1]
        local_experts = w_gate.shape[0]
        capacity = tok_dev * top_k // num_devices
        slots, slot_gates = routing_tables(expert_ids, gate_weights, num_devices, local_experts, capacity)
        slots = slots.reshape(dims[0], num_devices // dims[0], tok_dev)
        slot_gates = jnp.pad(slot_gates, ((0, 0), (0, 8 - local_experts), (0, 128 - capacity)))
        return moe_call(dims, tokens, slots, slot_gates, w_gate, w_up, w_down, capacity)

    return jax.shard_map(local_layer, mesh=mesh, in_specs=(row_spec, row_spec, row_spec, w_spec, w_spec, w_spec), out_specs=row_spec, check_vma=False)
```

```python
import functools
import math

import jax
import jax.numpy as jnp
from jax import lax
from jax.experimental import pallas as pl
from jax.experimental.pallas import tpu as pltpu
from jax.sharding import PartitionSpec as P

MESH = pl.DeviceIdType.MESH
F32 = jnp.float32
BF16 = jnp.bfloat16


def routing_tables(expert_ids, gate_weights, num_devices, local_experts, capacity):
    tok_dev = expert_ids.shape[0]
    dev_hit = jnp.any((expert_ids // local_experts)[:, :, None] == jnp.arange(num_devices)[None, None, :], axis=1)
    slot_pos = jnp.where(dev_hit, jnp.cumsum(dev_hit.astype(jnp.int32), axis=0) - 1, -1)
    all_experts = jnp.arange(num_devices * local_experts)
    gate_dense = jnp.sum(jnp.where(expert_ids[:, :, None] == all_experts[None, None, :], gate_weights[:, :, None], 0.0), axis=1)
    gate_dense = gate_dense.reshape(tok_dev, num_devices, local_experts)
    place = slot_pos[:, :, None] == jnp.arange(capacity)[None, None, :]
    slot_gates = jnp.sum(jnp.where(place[:, :, None, :], gate_dense[:, :, :, None], 0.0), axis=0)
    return slot_pos.T, slot_gates


ORDER = (
    "p00", "p01", "Y00", "X00", "p10", "X01", "Y01", "p11", "X11", "Y10", "c00", "X10", "p20", "Y20", "c01", "p21",
    "X20", "X21", "Y11", "c02", "c03", "p30", "Y21", "c10", "c11", "X30", "Y30", "c12", "p31", "c13", "y10", "X31",
    "x11", "c20", "c21", "Y31", "c22", "x10", "c23", "y11", "c30", "x21", "c31", "u11", "y21", "c32", "c33", "y31",
    "x31", "y30", "y01", "x30", "u10", "x20", "x01", "u21", "u31", "u30", "y20", "x00", "u20", "u01", "y00", "u00",
)


def moe_kernel(
    dims, x_ref, slot_ref, sgate_ref, w1_ref, w3_ref, w2_ref, out_ref,
    xall, smap, grecv, place, sbuf, drecv, rrecv, zret, acc, hbuf, gb, wb1, wb3, wb2,
    x_sem, w_sem, zs_send, zs_recv, sm_send, sm_recv, g_send, g_recv, d_send, d_recv, r_send, r_recv, zr_send, zr_recv,
):
    nz, ny, nx = dims
    nq = ny * nx
    ndev = nz * nq
    tok, hid = xall.shape[1:]
    cap = sbuf.shape[2]
    ff = wb1.shape[2]
    rows = nq * cap
    nt = 256
    ft = 256
    half = hid // 2
    z = lax.axis_index("ez")
    iy, ix = lax.axis_index("ey"), lax.axis_index("ex")
    q = iy * nx + ix
    me = z * nq + q
    col, core = lax.div(ix, 2), lax.rem(ix, 2)

    def at(zz, qq):
        return (zz, lax.div(qq, nx), lax.rem(qq, nx))

    def rcopy(src, dst, ss, rs, dev):
        return pltpu.make_async_remote_copy(src_ref=src, dst_ref=dst, send_sem=ss, recv_sem=rs, device_id=dev, device_id_type=MESH)

    inner = lax.div(z * (3 - z), 2)
    flip = lax.div(z, 2)

    def mirrored(b):
        return b + flip * (3 - 2 * b)

    k1, k2, k3 = mirrored(1 - inner), mirrored(2), mirrored(3)
    chunk = (z, k1, k2, k3)

    def plane_of(s):
        return (
            z * lax.div(3 - s, 3)
            + k1 * (lax.rem(s, 2) * lax.div(4 - s, 3))
            + k2 * ((1 - lax.rem(s, 2)) * lax.div(s, 2))
            + k3 * lax.div(s, 3)
        )

    def peer(f):
        fy, fx, fc = f // 4, (f // 2) % 2, f % 2
        return (iy + fy * (1 - 2 * iy)) * nx + (col + fx * (1 - 2 * col)) * 2 + core + fc * (1 - 2 * core)

    def hcols(h):
        return pl.ds(h * half, half)

    def tiles(h, body):
        @pl.loop(0, half // nt)
        def _(n):
            body(pl.ds(pl.multiple_of(h * half + n * nt, nt), nt))

    def weight_copies(e, slot):
        return (
            pltpu.make_async_copy(w1_ref.at[e], wb1.at[slot], w_sem.at[slot, 0]),
            pltpu.make_async_copy(w3_ref.at[e], wb3.at[slot], w_sem.at[slot, 1]),
            pltpu.make_async_copy(w2_ref.at[e], wb2.at[slot], w_sem.at[slot, 2]),
        )

    def z_rows(k, dst_z, n, h):
        ref = xall.at[k, :, hcols(h)]
        return rcopy(ref, ref, zs_send.at[n, h], zs_recv.at[k, h], at(dst_z, q))

    def z_wait(k, h):
        z_rows(k, z, 0, h).wait_recv()
        if h == 0:
            rcopy(smap.at[k], smap.at[k], sm_send.at[0], sm_recv.at[k], at(z, q)).wait_recv()

    def slot_copy(o):
        dz = lax.rem(z + o, nz)
        return rcopy(slot_ref.at[dz], smap.at[z], sm_send.at[o], sm_recv.at[z], at(dz, q))

    def gate_copy(o):
        d = lax.rem(me + o, ndev)
        return rcopy(sgate_ref.at[d], grecv.at[me], g_send.at[o], g_recv.at[me], at(lax.div(d, nq), lax.rem(d, nq)))

    def d_copy(s, h, f):
        k = chunk[s]
        return rcopy(sbuf.at[s % 2, peer(f), :, hcols(h)], drecv.at[k, q, :, hcols(h)], d_send.at[2 * (s % 2) + h, f], d_recv.at[2 * k + h, q], at(z, peer(f)))

    def r_copy(s, h, f):
        k = chunk[s]
        return rcopy(drecv.at[k, peer(f), :, hcols(h)], rrecv.at[k, q, :, hcols(h)], r_send.at[2 * s + h, f], r_recv.at[2 * k + h, q], at(z, peer(f)))

    def zr_copy(k, h, n, slot, dst_z):
        return rcopy(xall.at[k, :, hcols(h)], zret.at[slot, :, hcols(h)], zr_send.at[n, h], zr_recv.at[slot, h], at(dst_z, q))

    def zr_wait(slot, h):
        zr_copy(slot, h, 0, slot, z).wait_recv()

    def summed(k, cols):
        got = rrecv[k, :, :, cols].reshape(rows, nt)
        return lax.dot_general(place[k], got, (((0,), (0,)), ((), ())), preferred_element_type=F32)

    def pick(s, h):
        k = chunk[s]
        if s >= 1:
            if s == 1:
                z_wait(k1, h)

            @pl.when(inner == 1)
            def _():
                if s == 1:
                    z_wait(k2, h)
                    z_rows(k1, k2, 2, h).start()
                    z_rows(k2, k1, 3, h).start()
                if s == 2:
                    z_wait(k3, h)
                    z_rows(k3, k1, 4, h).start()

            if s >= 2:
                @pl.when(inner == 0)
                def _():
                    z_wait(k, h)
        if s >= 2:
            for f in range(1, nq):
                d_copy(s - 2, h, f).wait_send()
        if h == 0:
            lane_slot = lax.broadcasted_iota(jnp.int32, (cap, tok), 0)
            for d in range(nq):
                hit = lane_slot == smap[k, d : d + 1, :]
                place[k, d * cap : (d + 1) * cap, :] = jnp.where(hit, 1.0, 0.0).astype(BF16)

        def tile(cols):
            got = jnp.dot(place[k], xall[k, :, cols], preferred_element_type=F32).astype(BF16)
            sbuf[s % 2, :, :, cols] = got.reshape(nq, cap, nt)
            drecv[k, q, :, cols] = sbuf[s % 2, q, :, cols]

        tiles(h, tile)

    def send_picked(s, h, fs):
        for f in fs:
            d_copy(s, h, f).start()

    def d_wait(k):
        for f in range(1, nq):
            r = peer(f)
            for h in range(2):
                blk = drecv.at[k, r, :, hcols(h)]
                rcopy(blk, blk, d_send.at[0, f], d_recv.at[2 * k + h, r], at(z, q)).wait_recv()

    def send_back(s, h, fs):
        for f in fs:
            r_copy(s, h, f).start()
        if 1 in fs:
            def tile(cols):
                rrecv[chunk[s], q, :, cols] = drecv[chunk[s], q, :, cols]

            tiles(h, tile)

    def r_wait(k, h):
        for f in range(1, nq):
            r = peer(f)
            blk = rrecv.at[k, r, :, hcols(h)]
            rcopy(blk, blk, r_send.at[0, f], r_recv.at[2 * k + h, r], at(z, q)).wait_recv()

    def pass_on(s, h):
        k = chunk[s]
        r_wait(k, h)
        if s == 0:
            zr_wait(k1, h)
            zr_wait(k2, h)

            def tile(cols):
                total = summed(k, cols) + xall[k, :, cols].astype(F32)
                total = total + zret[k1, :, cols].astype(F32) + zret[k2, :, cols].astype(F32)
                out_ref[:, cols] = total.astype(BF16)

            tiles(h, tile)
            return

        @pl.when(inner == 1)
        def _():
            n, dst = ((2, k2), (3, k1), (4, k1))[s - 1]
            z_rows(k, dst, n, h).wait_send()

        def plain(cols):
            xall[k, :, cols] = summed(k, cols).astype(BF16)

        if s == 1:
            tiles(h, plain)
        else:
            slot = z if s == 2 else k

            @pl.when(inner == 1)
            def _():
                zr_wait(slot, h)

                def joined(cols):
                    xall[k, :, cols] = (summed(k, cols) + zret[slot, :, cols].astype(F32)).astype(BF16)

                tiles(h, joined)

            @pl.when(inner == 0)
            def _():
                tiles(h, plain)

        if s == 1:
            zr_copy(k, h, s, z, k).start()
        else:
            pl.when(inner == 1)(zr_copy(k, h, s, z, k).start)
            pl.when(inner == 0)(zr_copy(k, h, s, k1 if s == 2 else k, k1).start)

    def run(word):
        what, s, h = word[0], int(word[1]), int(word[2])
        if what == "p":
            pick(s, h)
        if what == "X":
            send_picked(s, h, (1, 2, 3, 6, 7))
        if what == "Y":
            send_picked(s, h, (4, 5))
        if what == "x":
            send_back(s, h, (1, 2, 3, 6, 7))
        if what == "y":
            send_back(s, h, (4, 5))
        if what == "u":
            pass_on(s, h)

    before, seen = {}, 0
    for word in ORDER:
        if word[0] == "c":
            seen += 1
        else:
            before.setdefault(seen, []).append(word)

    load_x = pltpu.make_async_copy(x_ref, xall.at[z], x_sem)
    load_x.start()
    for o in range(1, nz):
        slot_copy(o).start()
    for c in weight_copies(0, 0):
        c.start()
    load_x.wait()
    for h in range(2):
        @pl.when(z > 0)
        def _():
            z_rows(z, z - 1, 0, h).start()

        @pl.when(z < nz - 1)
        def _():
            z_rows(z, z + 1, 1, h).start()

    smap[z] = slot_ref[z]
    for word in before.get(0, ()):
        run(word)
        if word == "X00":
            for o in range(1, ndev):
                gate_copy(o).start()
            grecv[me] = sgate_ref[me]
    for o in range(1, ndev):
        s = lax.rem(me + o, ndev)
        rcopy(sgate_ref.at[0], grecv.at[s], g_send.at[o], g_recv.at[s], at(z, q)).wait_recv()

    def expert_step(i, _):
        s, e, slot = lax.div(i, 4), lax.rem(i, 4), lax.rem(i, 2)
        k = plane_of(s)

        for n in range(1, 16):
            if n in before:
                @pl.when(i == n)
                def _():
                    for word in before[n]:
                        run(word)

        @pl.when(i < 15)
        def _():
            for c in weight_copies(lax.rem(i + 1, 4), 1 - slot):
                c.start()

        @pl.when(e == 0)
        def _():
            d_wait(k)
            by_slot = grecv[pl.ds(k * nq, nq)].reshape(nq * 8, 128).T
            for r in range(nq):
                for j in range(4):
                    one = by_slot[0:cap, r * 8 + j : r * 8 + j + 1]
                    gb[j, r * cap : (r + 1) * cap, :] = jnp.broadcast_to(one, (cap, 128))

        for c in weight_copies(e, slot):
            c.wait()

        @pl.loop(0, ff // ft)
        def _(n):
            cols = pl.ds(pl.multiple_of(n * ft, ft), ft)
            xin = drecv[k].reshape(rows, hid)
            a = jnp.dot(xin, wb1[slot, :, cols], preferred_element_type=F32)
            b = jnp.dot(xin, wb3[slot, :, cols], preferred_element_type=F32)
            hbuf[:, cols] = (a * jax.nn.sigmoid(a) * b).astype(BF16)

        @pl.loop(0, hid // nt)
        def _(n):
            cols = pl.ds(pl.multiple_of(n * nt, nt), nt)
            o = jnp.dot(hbuf[...], wb2[slot, :, cols], preferred_element_type=F32)
            g = jnp.concatenate([gb[e]] * (nt // 128), axis=1)
            term = jnp.where(g > 0.0, o * g, 0.0)
            acc[:, cols] = jnp.where(e == 0, 0.0, acc[:, cols]) + term

        @pl.when(e == 3)
        def _():
            @pl.loop(0, hid // nt)
            def _(n):
                cols = pl.ds(pl.multiple_of(n * nt, nt), nt)
                drecv[k, :, :, cols] = acc[:, cols].astype(BF16).reshape(nq, cap, nt)

        return 0

    lax.fori_loop(0, 16, expert_step, 0)
    for word in before.get(16, ()):
        run(word)

    for h in range(2):
        @pl.when(z > 0)
        def _():
            z_rows(z, z - 1, 0, h).wait_send()

        @pl.when(z < nz - 1)
        def _():
            z_rows(z, z + 1, 1, h).wait_send()

        for s in range(1, 4):
            zr_copy(chunk[s], h, s, z, k1).wait_send()
        for f in range(1, nq):
            for s in range(4):
                r_copy(s, h, f).wait_send()
                if s >= 2:
                    d_copy(s, h, f).wait_send()
    for o in range(1, nz):
        slot_copy(o).wait_send()
    for o in range(1, ndev):
        gate_copy(o).wait_send()


def moe_call(dims, x, slots, slot_gates, w1, w3, w2, capacity):
    nz, ny, nx = dims
    nq = ny * nx
    ndev = nz * nq
    tok, hid = x.shape
    ff = w1.shape[2]
    dma = pltpu.SemaphoreType.DMA
    vmem = pl.BlockSpec(memory_space=pltpu.VMEM)
    hbm = pl.BlockSpec(memory_space=pl.ANY)
    return pl.pallas_call(
        functools.partial(moe_kernel, dims),
        out_shape=jax.ShapeDtypeStruct((tok, hid), BF16),
        in_specs=[hbm, vmem, vmem, hbm, hbm, hbm],
        out_specs=vmem,
        scratch_shapes=[
            pltpu.VMEM((nz, tok, hid), BF16),
            pltpu.VMEM((nz, nq, tok), jnp.int32),
            pltpu.VMEM((ndev, 8, 128), F32),
            pltpu.VMEM((nz, nq * capacity, tok), BF16),
            pltpu.VMEM((2, nq, capacity, hid), BF16),
            pltpu.VMEM((nz, nq, capacity, hid), BF16),
            pltpu.VMEM((nz, nq, capacity, hid), BF16),
            pltpu.VMEM((nz, tok, hid), BF16),
            pltpu.VMEM((nq * capacity, hid), F32),
            pltpu.VMEM((nq * capacity, ff), BF16),
            pltpu.VMEM((4, nq * capacity, 128), F32),
            pltpu.VMEM((2, hid, ff), BF16),
            pltpu.VMEM((2, hid, ff), BF16),
            pltpu.VMEM((2, ff, hid), BF16),
            dma,
            dma((2, 3)),
            dma((5, 2)),
            dma((nz, 2)),
            dma((nz,)),
            dma((nz,)),
            dma((ndev,)),
            dma((ndev,)),
            dma((4, nq)),
            dma((2 * nz, nq)),
            dma((2 * nz, nq)),
            dma((2 * nz, nq)),
            dma((nz, 2)),
            dma((nz, 2)),
        ],
        compiler_params=pltpu.CompilerParams(has_side_effects=True, vmem_limit_bytes=66 * 1000 * 1000),
    )(x, slots, slot_gates, w1, w3, w2)


def solution(mesh):
    ep_axes = tuple(mesh.axis_names)
    dims = tuple(mesh.shape[axis_name] for axis_name in ep_axes)
    num_devices = math.prod(dims)
    row_spec = P(ep_axes, None)
    w_spec = P(ep_axes, None, None)

    def local_layer(tokens, expert_ids, gate_weights, w_gate, w_up, w_down):
        tok_dev = tokens.shape[0]
        top_k = expert_ids.shape[1]
        local_experts = w_gate.shape[0]
        capacity = tok_dev * top_k // num_devices
        slots, slot_gates = routing_tables(expert_ids, gate_weights, num_devices, local_experts, capacity)
        slots = slots.reshape(dims[0], num_devices // dims[0], tok_dev)
        slot_gates = jnp.pad(slot_gates, ((0, 0), (0, 8 - local_experts), (0, 128 - capacity)))
        return moe_call(dims, tokens, slots, slot_gates, w_gate, w_up, w_down, capacity)

    return jax.shard_map(local_layer, mesh=mesh, in_specs=(row_spec, row_spec, row_spec, w_spec, w_spec, w_spec), out_specs=row_spec, check_vma=False)
```

```python
import functools
import math

import jax
import jax.numpy as jnp
from jax import lax
from jax.experimental import pallas as pl
from jax.experimental.pallas import tpu as pltpu
from jax.sharding import PartitionSpec as P

MESH = pl.DeviceIdType.MESH
F32 = jnp.float32
BF16 = jnp.bfloat16


ORDER = (
    "p00", "p01", "X00", "Y00", "G01", "p10", "G10", "G00", "p11", "X01", "G11", "Y01", "X10", "p20", "X11", "Y20",
    "c00", "Y10", "Y11", "c01", "X20", "p21", "c02", "G21", "G20", "c03", "c10", "p30", "G30", "c11", "Y21", "X21",
    "p31", "G31", "c12", "c13", "Y30", "x10", "X31", "y01", "X30", "Y31", "c20", "g10", "c21", "g11", "y10", "c22",
    "c23", "c30", "c31", "g21", "c32", "x21", "u10", "y21", "c33", "x31", "x30", "g30", "g31", "x20", "y30", "u21",
    "g20", "y11", "x11", "u30", "x00", "y31", "y20", "g00", "u31", "g01", "u20", "y00", "u11", "x01", "u00", "u01",
)


def moe_kernel(
    dims, x_ref, ids_ref, gates_ref, w1_ref, w3_ref, w2_ref, out_ref,
    slot_ref, sgate_ref, dense, xall, smap, grecv, place, sbuf, drecv, rrecv, zret, acc, hbuf, gb, wb1, wb3, wb2,
    x_sem, w_sem, zs_send, zs_recv, sm_send, sm_recv, g_send, g_recv, d_send, d_recv, r_send, r_recv, zr_send, zr_recv,
):
    nz, ny, nx = dims
    nq = ny * nx
    ndev = nz * nq
    tok, hid = xall.shape[1:]
    cap = sbuf.shape[2]
    ff = wb1.shape[2]
    rows = nq * cap
    nt = 256
    ft = 256
    ot = 256
    half = hid // 2
    z = lax.axis_index("ez")
    iy, ix = lax.axis_index("ey"), lax.axis_index("ex")
    q = iy * nx + ix
    me = z * nq + q
    col, core = lax.div(ix, 2), lax.rem(ix, 2)

    def at(zz, qq):
        return (zz, lax.div(qq, nx), lax.rem(qq, nx))

    def rcopy(src, dst, ss, rs, dev):
        return pltpu.make_async_remote_copy(src_ref=src, dst_ref=dst, send_sem=ss, recv_sem=rs, device_id=dev, device_id_type=MESH)

    inner = lax.div(z * (3 - z), 2)
    flip = lax.div(z, 2)

    def mirrored(b):
        return b + flip * (3 - 2 * b)

    k1, k2, k3 = mirrored(1 - inner), mirrored(2), mirrored(3)
    chunk = (z, k1, k2, k3)

    def plane_of(s):
        return (
            z * lax.div(3 - s, 3)
            + k1 * (lax.rem(s, 2) * lax.div(4 - s, 3))
            + k2 * ((1 - lax.rem(s, 2)) * lax.div(s, 2))
            + k3 * lax.div(s, 3)
        )

    def peer(f):
        fy, fx, fc = f // 4, (f // 2) % 2, f % 2
        return (iy + fy * (1 - 2 * iy)) * nx + (col + fx * (1 - 2 * col)) * 2 + core + fc * (1 - 2 * core)

    def hcols(h):
        return pl.ds(h * half, half)

    def tiles(h, body):
        @pl.loop(0, half // nt)
        def _(n):
            body(pl.ds(pl.multiple_of(h * half + n * nt, nt), nt))

    def weight_copies(e, slot):
        return (
            pltpu.make_async_copy(w1_ref.at[e], wb1.at[slot], w_sem.at[slot, 0]),
            pltpu.make_async_copy(w3_ref.at[e], wb3.at[slot], w_sem.at[slot, 1]),
            pltpu.make_async_copy(w2_ref.at[e], wb2.at[slot], w_sem.at[slot, 2]),
        )

    def z_rows(k, dst_z, n, h):
        ref = xall.at[k, :, hcols(h)]
        return rcopy(ref, ref, zs_send.at[n, h], zs_recv.at[k, h], at(dst_z, q))

    def z_wait(k, h):
        z_rows(k, z, 0, h).wait_recv()
        if h == 0:
            rcopy(smap.at[k], smap.at[k], sm_send.at[0], sm_recv.at[k], at(z, q)).wait_recv()

    def slot_copy(o):
        dz = lax.rem(z + o, nz)
        return rcopy(slot_ref.at[dz], smap.at[z], sm_send.at[o], sm_recv.at[z], at(dz, q))

    def gate_copy(o):
        d = lax.rem(me + o, ndev)
        return rcopy(sgate_ref.at[d], grecv.at[me], g_send.at[o], g_recv.at[me], at(lax.div(d, nq), lax.rem(d, nq)))

    def d_copy(s, h, f):
        k = chunk[s]
        return rcopy(sbuf.at[s % 2, peer(f), :, hcols(h)], drecv.at[k, q, :, hcols(h)], d_send.at[2 * (s % 2) + h, f], d_recv.at[2 * k + h, q], at(z, peer(f)))

    def r_copy(s, h, f):
        k = chunk[s]
        return rcopy(drecv.at[k, peer(f), :, hcols(h)], rrecv.at[k, q, :, hcols(h)], r_send.at[2 * s + h, f], r_recv.at[2 * k + h, q], at(z, peer(f)))

    def zr_copy(k, h, n, slot, dst_z):
        return rcopy(xall.at[k, :, hcols(h)], zret.at[slot, :, hcols(h)], zr_send.at[n, h], zr_recv.at[slot, h], at(dst_z, q))

    def zr_wait(slot, h):
        zr_copy(slot, h, 0, slot, z).wait_recv()

    def summed(k, cols):
        got = rrecv[k, :, :, cols].reshape(rows, nt)
        return lax.dot_general(place[k], got, (((0,), (0,)), ((), ())), preferred_element_type=F32)

    def pick(s, h):
        k = chunk[s]
        if s >= 1:
            if s == 1:
                z_wait(k1, h)

            @pl.when(inner == 1)
            def _():
                if s == 1:
                    z_wait(k2, h)
                    z_rows(k1, k2, 2, h).start()
                    z_rows(k2, k1, 3, h).start()
                if s == 2:
                    z_wait(k3, h)
                    z_rows(k3, k1, 4, h).start()

            if s >= 2:
                @pl.when(inner == 0)
                def _():
                    z_wait(k, h)
        if s >= 2:
            for f in range(1, nq):
                d_copy(s - 2, h, f).wait_send()
        if h == 0:
            lane_slot = lax.broadcasted_iota(jnp.int32, (cap, tok), 0)
            for d in range(nq):
                hit = lane_slot == smap[k, d : d + 1, :]
                place[k, d * cap : (d + 1) * cap, :] = jnp.where(hit, 1.0, 0.0).astype(BF16)

        def tile(cols):
            got = jnp.dot(place[k], xall[k, :, cols], preferred_element_type=F32).astype(BF16)
            sbuf[s % 2, :, :, cols] = got.reshape(nq, cap, nt)
            drecv[k, q, :, cols] = sbuf[s % 2, q, :, cols]

        tiles(h, tile)

    def send_picked(s, h, fs):
        for f in fs:
            d_copy(s, h, f).start()

    def d_wait(k):
        for f in range(1, nq):
            r = peer(f)
            for h in range(2):
                blk = drecv.at[k, r, :, hcols(h)]
                rcopy(blk, blk, d_send.at[0, f], d_recv.at[2 * k + h, r], at(z, q)).wait_recv()

    def send_back(s, h, fs):
        for f in fs:
            r_copy(s, h, f).start()
        if 1 in fs:
            def tile(cols):
                rrecv[chunk[s], q, :, cols] = drecv[chunk[s], q, :, cols]

            tiles(h, tile)

    def r_wait(k, h):
        for f in range(1, nq):
            r = peer(f)
            blk = rrecv.at[k, r, :, hcols(h)]
            rcopy(blk, blk, r_send.at[0, f], r_recv.at[2 * k + h, r], at(z, q)).wait_recv()

    def pass_on(s, h):
        k = chunk[s]
        r_wait(k, h)
        if s == 0:
            zr_wait(k1, h)
            zr_wait(k2, h)

            def tile(cols):
                total = summed(k, cols) + xall[k, :, cols].astype(F32)
                total = total + zret[k1, :, cols].astype(F32) + zret[k2, :, cols].astype(F32)
                out_ref[:, cols] = total.astype(BF16)

            tiles(h, tile)
            return

        @pl.when(inner == 1)
        def _():
            n, dst = ((2, k2), (3, k1), (4, k1))[s - 1]
            z_rows(k, dst, n, h).wait_send()

        def plain(cols):
            xall[k, :, cols] = summed(k, cols).astype(BF16)

        if s == 1:
            tiles(h, plain)
        else:
            slot = z if s == 2 else k

            @pl.when(inner == 1)
            def _():
                zr_wait(slot, h)

                def joined(cols):
                    xall[k, :, cols] = (summed(k, cols) + zret[slot, :, cols].astype(F32)).astype(BF16)

                tiles(h, joined)

            @pl.when(inner == 0)
            def _():
                tiles(h, plain)

        if s == 1:
            zr_copy(k, h, s, z, k).start()
        else:
            pl.when(inner == 1)(zr_copy(k, h, s, z, k).start)
            pl.when(inner == 0)(zr_copy(k, h, s, k1 if s == 2 else k, k1).start)

    def slot_table():
        device = lax.broadcasted_iota(jnp.int32, (ndev, tok), 0)
        hit = None
        for j in range(ids_ref.shape[0]):
            here = lax.shift_right_logical(ids_ref[j : j + 1, :], 2) == device
            hit = here if hit is None else jnp.logical_or(hit, here)
        hit = jnp.where(hit, 1.0, 0.0)
        upto = lax.broadcasted_iota(jnp.int32, (tok, tok), 0) <= lax.broadcasted_iota(jnp.int32, (tok, tok), 1)
        upto = jnp.where(upto, 1.0, 0.0).astype(BF16)
        count = jnp.dot(hit.astype(BF16), upto, preferred_element_type=F32)
        slot = jnp.where(hit > 0.0, count - 1.0, -1.0).astype(jnp.int32)
        slot_ref[...] = slot.reshape(nz, nq, tok)

    def gate_table():
        row = lax.broadcasted_iota(jnp.int32, (ndev * 8, tok), 0)
        low = jnp.bitwise_and(row, 7)
        expert = jnp.where(low < 4, lax.shift_right_logical(row, 3) * 4 + low, -1)
        gate = jnp.zeros((ndev * 8, tok), F32)
        for j in range(ids_ref.shape[0]):
            gate = gate + jnp.where(ids_ref[j : j + 1, :] == expert, gates_ref[j : j + 1, :], 0.0)
        dense[...] = gate

        @pl.loop(0, ndev, unroll=4)
        def _(d):
            g = dense[pl.ds(pl.multiple_of(d * 8, 8), 8), :]
            hi = g.astype(BF16).astype(F32)
            mid = (g - hi).astype(BF16).astype(F32)
            low = g - hi - mid
            parts = jnp.concatenate([hi, mid, low, jnp.zeros_like(g)], axis=0).astype(BF16)
            slot = slot_ref[lax.div(d, nq), pl.ds(lax.rem(d, nq), 1), :]
            spot = lax.broadcasted_iota(jnp.int32, (128, tok), 0) == slot
            spot = jnp.where(spot, 1.0, 0.0).astype(BF16)
            got = lax.dot_general(parts, spot, (((1,), (1,)), ((), ())), preferred_element_type=F32)
            sgate_ref[d] = got[0:8] + got[8:16] + got[16:24]

    def run(word):
        what, s, h = word[0], int(word[1]), int(word[2])
        if what == "p":
            pick(s, h)
        if what == "X":
            send_picked(s, h, (1, 2, 3))
        if what == "G":
            send_picked(s, h, (6, 7))
        if what == "Y":
            send_picked(s, h, (4, 5))
        if what == "x":
            send_back(s, h, (1, 2, 3))
        if what == "g":
            send_back(s, h, (6, 7))
        if what == "y":
            send_back(s, h, (4, 5))
        if what == "u":
            pass_on(s, h)

    before, seen = {}, 0
    for word in ORDER:
        if word[0] == "c":
            seen += 1
        else:
            before.setdefault(seen, []).append(word)

    load_x = pltpu.make_async_copy(x_ref, xall.at[z], x_sem)
    load_x.start()
    for c in weight_copies(0, 0):
        c.start()
    slot_table()
    for o in range(1, nz):
        slot_copy(o).start()
    load_x.wait()
    for h in range(2):
        @pl.when(z > 0)
        def _():
            z_rows(z, z - 1, 0, h).start()

        @pl.when(z < nz - 1)
        def _():
            z_rows(z, z + 1, 1, h).start()

    smap[z] = slot_ref[z]
    gates_sent = False
    for word in before.get(0, ()):
        if word[:2] == "p1" and not gates_sent:
            gates_sent = True
            gate_table()
            for o in range(1, ndev):
                gate_copy(o).start()
            grecv[me] = sgate_ref[me]
        run(word)
    for o in range(1, ndev):
        s = lax.rem(me + o, ndev)
        rcopy(sgate_ref.at[0], grecv.at[s], g_send.at[o], g_recv.at[s], at(z, q)).wait_recv()

    def expert_step(i, _):
        s, e, slot = lax.div(i, 4), lax.rem(i, 4), lax.rem(i, 2)
        k = plane_of(s)

        for n in range(1, 16):
            if n in before:
                @pl.when(i == n)
                def _():
                    for word in before[n]:
                        run(word)

        @pl.when(i < 15)
        def _():
            for c in weight_copies(lax.rem(i + 1, 4), 1 - slot):
                c.start()

        @pl.when(e == 0)
        def _():
            d_wait(k)
            by_slot = grecv[pl.ds(k * nq, nq)].reshape(nq * 8, 128).T
            for r in range(nq):
                for j in range(4):
                    one = by_slot[0:cap, r * 8 + j : r * 8 + j + 1]
                    gb[j, r * cap : (r + 1) * cap, :] = jnp.broadcast_to(one, (cap, 128))

        for c in weight_copies(e, slot):
            c.wait()

        @pl.loop(0, ff // ft, unroll=3)
        def _(n):
            cols = pl.ds(pl.multiple_of(n * ft, ft), ft)
            xin = drecv[k].reshape(rows, hid)
            a = jnp.dot(xin, wb1[slot, :, cols], preferred_element_type=F32)
            b = jnp.dot(xin, wb3[slot, :, cols], preferred_element_type=F32)
            hbuf[:, cols] = (a * jax.nn.sigmoid(a) * b).astype(BF16)

        @pl.loop(0, hid // ot, unroll=8)
        def _(n):
            cols = pl.ds(pl.multiple_of(n * ot, ot), ot)
            o = jnp.dot(hbuf[...], wb2[slot, :, cols], preferred_element_type=F32)
            g = jnp.concatenate([gb[e]] * (ot // 128), axis=1)
            term = jnp.where(g > 0.0, o * g, 0.0)
            acc[:, cols] = jnp.where(e == 0, 0.0, acc[:, cols]) + term

        @pl.when(e == 3)
        def _():
            @pl.loop(0, hid // nt)
            def _(n):
                cols = pl.ds(pl.multiple_of(n * nt, nt), nt)
                drecv[k, :, :, cols] = acc[:, cols].astype(BF16).reshape(nq, cap, nt)

        return 0

    lax.fori_loop(0, 16, expert_step, 0)
    for word in before.get(16, ()):
        run(word)

    for h in range(2):
        @pl.when(z > 0)
        def _():
            z_rows(z, z - 1, 0, h).wait_send()

        @pl.when(z < nz - 1)
        def _():
            z_rows(z, z + 1, 1, h).wait_send()

        for s in range(1, 4):
            zr_copy(chunk[s], h, s, z, k1).wait_send()
        for f in range(1, nq):
            for s in range(4):
                r_copy(s, h, f).wait_send()
                if s >= 2:
                    d_copy(s, h, f).wait_send()
    for o in range(1, nz):
        slot_copy(o).wait_send()
    for o in range(1, ndev):
        gate_copy(o).wait_send()


def moe_call(dims, x, ids, gates, w1, w3, w2, capacity):
    nz, ny, nx = dims
    nq = ny * nx
    ndev = nz * nq
    tok, hid = x.shape
    ff = w1.shape[2]
    dma = pltpu.SemaphoreType.DMA
    vmem = pl.BlockSpec(memory_space=pltpu.VMEM)
    hbm = pl.BlockSpec(memory_space=pl.ANY)
    return pl.pallas_call(
        functools.partial(moe_kernel, dims),
        out_shape=jax.ShapeDtypeStruct((tok, hid), BF16),
        in_specs=[hbm, vmem, vmem, hbm, hbm, hbm],
        out_specs=vmem,
        scratch_shapes=[
            pltpu.VMEM((nz, nq, tok), jnp.int32),
            pltpu.VMEM((ndev, 8, 128), F32),
            pltpu.VMEM((ndev * 8, tok), F32),
            pltpu.VMEM((nz, tok, hid), BF16),
            pltpu.VMEM((nz, nq, tok), jnp.int32),
            pltpu.VMEM((ndev, 8, 128), F32),
            pltpu.VMEM((nz, nq * capacity, tok), BF16),
            pltpu.VMEM((2, nq, capacity, hid), BF16),
            pltpu.VMEM((nz, nq, capacity, hid), BF16),
            pltpu.VMEM((nz, nq, capacity, hid), BF16),
            pltpu.VMEM((nz, tok, hid), BF16),
            pltpu.VMEM((nq * capacity, hid), F32),
            pltpu.VMEM((nq * capacity, ff), BF16),
            pltpu.VMEM((4, nq * capacity, 128), F32),
            pltpu.VMEM((2, hid, ff), BF16),
            pltpu.VMEM((2, hid, ff), BF16),
            pltpu.VMEM((2, ff, hid), BF16),
            dma,
            dma((2, 3)),
            dma((5, 2)),
            dma((nz, 2)),
            dma((nz,)),
            dma((nz,)),
            dma((ndev,)),
            dma((ndev,)),
            dma((4, nq)),
            dma((2 * nz, nq)),
            dma((2 * nz, nq)),
            dma((2 * nz, nq)),
            dma((nz, 2)),
            dma((nz, 2)),
        ],
        compiler_params=pltpu.CompilerParams(has_side_effects=True, vmem_limit_bytes=66 * 1000 * 1000),
    )(x, ids, gates, w1, w3, w2)


def solution(mesh):
    ep_axes = tuple(mesh.axis_names)
    dims = tuple(mesh.shape[axis_name] for axis_name in ep_axes)
    num_devices = math.prod(dims)
    row_spec = P(ep_axes, None)
    w_spec = P(ep_axes, None, None)

    def local_layer(tokens, expert_ids, gate_weights, w_gate, w_up, w_down):
        tok_dev = tokens.shape[0]
        top_k = expert_ids.shape[1]
        capacity = tok_dev * top_k // num_devices
        return moe_call(dims, tokens, expert_ids.T, gate_weights.T, w_gate, w_up, w_down, capacity)

    return jax.shard_map(local_layer, mesh=mesh, in_specs=(row_spec, row_spec, row_spec, w_spec, w_spec, w_spec), out_specs=row_spec, check_vma=False)
```

```python
import functools
import math

import jax
import jax.numpy as jnp
from jax import lax
from jax.experimental import pallas as pl
from jax.experimental.pallas import tpu as pltpu
from jax.sharding import PartitionSpec as P

MESH = pl.DeviceIdType.MESH
F32 = jnp.float32
BF16 = jnp.bfloat16


ORDER = (
    "p00", "p01", "X00", "Y00", "G01", "p10", "G10", "G00", "p11", "X01", "G11", "Y01", "X10", "p20", "X11", "Y20",
    "c00", "Y10", "Y11", "c01", "X20", "p21", "c02", "G21", "G20", "c03", "c10", "p30", "G30", "c11", "Y21", "X21",
    "p31", "G31", "c12", "c13", "Y30", "x10", "X31", "y01", "X30", "Y31", "c20", "g10", "c21", "g11", "y10", "c22",
    "c23", "c30", "c31", "g21", "c32", "x21", "u10", "y21", "c33", "x31", "x30", "g30", "g31", "x20", "y30", "u21",
    "g20", "y11", "x11", "u30", "x00", "y31", "y20", "g00", "u31", "g01", "u20", "y00", "u11", "x01", "u00", "u01",
)


def moe_kernel(
    dims, x_ref, ids_ref, gates_ref, w1_ref, w3_ref, w2_ref, out_ref,
    slot_ref, sgate_ref, dense, xall, smap, grecv, place, sbuf, drecv, rrecv, zret, acc, hbuf, gb, wb1, wb3, wb2,
    x_sem, w_sem, zs_send, zs_recv, sm_send, sm_recv, g_send, g_recv, d_send, d_recv, r_send, r_recv, zr_send, zr_recv,
):
    nz, ny, nx = dims
    nq = ny * nx
    ndev = nz * nq
    tok, hid = xall.shape[1:]
    cap = sbuf.shape[2]
    ff = wb1.shape[2]
    rows = nq * cap
    nt = 256
    ft = 256
    ot = 256
    half = hid // 2
    z = lax.axis_index("ez")
    iy, ix = lax.axis_index("ey"), lax.axis_index("ex")
    q = iy * nx + ix
    me = z * nq + q
    col, core = lax.div(ix, 2), lax.rem(ix, 2)

    def at(zz, qq):
        return (zz, lax.div(qq, nx), lax.rem(qq, nx))

    def rcopy(src, dst, ss, rs, dev):
        return pltpu.make_async_remote_copy(src_ref=src, dst_ref=dst, send_sem=ss, recv_sem=rs, device_id=dev, device_id_type=MESH)

    inner = lax.div(z * (3 - z), 2)
    flip = lax.div(z, 2)

    def mirrored(b):
        return b + flip * (3 - 2 * b)

    k1, k2, k3 = mirrored(1 - inner), mirrored(2), mirrored(3)
    chunk = (z, k1, k2, k3)

    def plane_of(s):
        return (
            z * lax.div(3 - s, 3)
            + k1 * (lax.rem(s, 2) * lax.div(4 - s, 3))
            + k2 * ((1 - lax.rem(s, 2)) * lax.div(s, 2))
            + k3 * lax.div(s, 3)
        )

    def peer(f):
        fy, fx, fc = f // 4, (f // 2) % 2, f % 2
        return (iy + fy * (1 - 2 * iy)) * nx + (col + fx * (1 - 2 * col)) * 2 + core + fc * (1 - 2 * core)

    def hcols(h):
        return pl.ds(h * half, half)

    def tiles(h, body):
        @pl.loop(0, half // nt)
        def _(n):
            body(pl.ds(pl.multiple_of(h * half + n * nt, nt), nt))

    def weight_copies(e, slot):
        return (
            pltpu.make_async_copy(w1_ref.at[e], wb1.at[slot], w_sem.at[slot, 0]),
            pltpu.make_async_copy(w3_ref.at[e], wb3.at[slot], w_sem.at[slot, 1]),
            pltpu.make_async_copy(w2_ref.at[e], wb2.at[slot], w_sem.at[slot, 2]),
        )

    def z_rows(k, dst_z, n, h):
        ref = xall.at[k, :, hcols(h)]
        return rcopy(ref, ref, zs_send.at[n, h], zs_recv.at[k, h], at(dst_z, q))

    def z_wait(k, h):
        z_rows(k, z, 0, h).wait_recv()
        if h == 0:
            rcopy(smap.at[k], smap.at[k], sm_send.at[0], sm_recv.at[k], at(z, q)).wait_recv()

    def slot_copy(o):
        dz = lax.rem(z + o, nz)
        return rcopy(slot_ref.at[dz], smap.at[z], sm_send.at[o], sm_recv.at[z], at(dz, q))

    def gate_copy(o):
        d = lax.rem(me + o, ndev)
        return rcopy(sgate_ref.at[d], grecv.at[me], g_send.at[o], g_recv.at[me], at(lax.div(d, nq), lax.rem(d, nq)))

    def d_copy(s, h, f):
        k = chunk[s]
        return rcopy(sbuf.at[s % 2, peer(f), :, hcols(h)], drecv.at[k, q, :, hcols(h)], d_send.at[2 * (s % 2) + h, f], d_recv.at[2 * k + h, q], at(z, peer(f)))

    def r_copy(s, h, f):
        k = chunk[s]
        return rcopy(drecv.at[k, peer(f), :, hcols(h)], rrecv.at[k, q, :, hcols(h)], r_send.at[2 * s + h, f], r_recv.at[2 * k + h, q], at(z, peer(f)))

    def zr_copy(k, h, n, slot, dst_z):
        return rcopy(xall.at[k, :, hcols(h)], zret.at[slot, :, hcols(h)], zr_send.at[n, h], zr_recv.at[slot, h], at(dst_z, q))

    def zr_wait(slot, h):
        zr_copy(slot, h, 0, slot, z).wait_recv()

    def summed(k, cols):
        got = rrecv[k, :, :, cols].reshape(rows, nt)
        return lax.dot_general(place[k], got, (((0,), (0,)), ((), ())), preferred_element_type=F32)

    def pick(s, h):
        k = chunk[s]
        if s >= 1:
            if s == 1:
                z_wait(k1, h)

            @pl.when(inner == 1)
            def _():
                if s == 1:
                    z_wait(k2, h)
                    z_rows(k1, k2, 2, h).start()
                    z_rows(k2, k1, 3, h).start()
                if s == 2:
                    z_wait(k3, h)
                    z_rows(k3, k1, 4, h).start()

            if s >= 2:
                @pl.when(inner == 0)
                def _():
                    z_wait(k, h)
        if s >= 2:
            for f in range(1, nq):
                d_copy(s - 2, h, f).wait_send()
        if h == 0:
            lane_slot = lax.broadcasted_iota(jnp.int32, (cap, tok), 0)
            for d in range(nq):
                hit = lane_slot == smap[k, d : d + 1, :]
                place[k, d * cap : (d + 1) * cap, :] = jnp.where(hit, 1.0, 0.0).astype(BF16)

        def tile(cols):
            got = jnp.dot(place[k], xall[k, :, cols], preferred_element_type=F32).astype(BF16)
            sbuf[s % 2, :, :, cols] = got.reshape(nq, cap, nt)
            drecv[k, q, :, cols] = sbuf[s % 2, q, :, cols]

        tiles(h, tile)

    def send_picked(s, h, fs):
        for f in fs:
            d_copy(s, h, f).start()

    def d_wait(k):
        for f in range(1, nq):
            r = peer(f)
            for h in range(2):
                blk = drecv.at[k, r, :, hcols(h)]
                rcopy(blk, blk, d_send.at[0, f], d_recv.at[2 * k + h, r], at(z, q)).wait_recv()

    def send_back(s, h, fs):
        for f in fs:
            r_copy(s, h, f).start()
        if 1 in fs:
            def tile(cols):
                rrecv[chunk[s], q, :, cols] = drecv[chunk[s], q, :, cols]

            tiles(h, tile)

    def r_wait(k, h):
        for f in range(1, nq):
            r = peer(f)
            blk = rrecv.at[k, r, :, hcols(h)]
            rcopy(blk, blk, r_send.at[0, f], r_recv.at[2 * k + h, r], at(z, q)).wait_recv()

    def pass_on(s, h):
        k = chunk[s]
        r_wait(k, h)
        if s == 0:
            zr_wait(k1, h)
            zr_wait(k2, h)

            def tile(cols):
                total = summed(k, cols) + xall[k, :, cols].astype(F32)
                total = total + zret[k1, :, cols].astype(F32) + zret[k2, :, cols].astype(F32)
                out_ref[:, cols] = total.astype(BF16)

            tiles(h, tile)
            return

        @pl.when(inner == 1)
        def _():
            n, dst = ((2, k2), (3, k1), (4, k1))[s - 1]
            z_rows(k, dst, n, h).wait_send()

        def plain(cols):
            xall[k, :, cols] = summed(k, cols).astype(BF16)

        if s == 1:
            tiles(h, plain)
        else:
            slot = z if s == 2 else k

            @pl.when(inner == 1)
            def _():
                zr_wait(slot, h)

                def joined(cols):
                    xall[k, :, cols] = (summed(k, cols) + zret[slot, :, cols].astype(F32)).astype(BF16)

                tiles(h, joined)

            @pl.when(inner == 0)
            def _():
                tiles(h, plain)

        if s == 1:
            zr_copy(k, h, s, z, k).start()
        else:
            pl.when(inner == 1)(zr_copy(k, h, s, z, k).start)
            pl.when(inner == 0)(zr_copy(k, h, s, k1 if s == 2 else k, k1).start)

    def slot_table():
        device = lax.broadcasted_iota(jnp.int32, (ndev, tok), 0)
        hit = None
        for j in range(ids_ref.shape[0]):
            here = lax.shift_right_logical(ids_ref[j : j + 1, :], 2) == device
            hit = here if hit is None else jnp.logical_or(hit, here)
        hit = jnp.where(hit, 1.0, 0.0)
        upto = lax.broadcasted_iota(jnp.int32, (tok, tok), 0) <= lax.broadcasted_iota(jnp.int32, (tok, tok), 1)
        upto = jnp.where(upto, 1.0, 0.0).astype(BF16)
        count = jnp.dot(hit.astype(BF16), upto, preferred_element_type=F32)
        slot = jnp.where(hit > 0.0, count - 1.0, -1.0).astype(jnp.int32)
        slot_ref[...] = slot.reshape(nz, nq, tok)

    def gate_table():
        row = lax.broadcasted_iota(jnp.int32, (ndev * 8, tok), 0)
        low = jnp.bitwise_and(row, 7)
        expert = jnp.where(low < 4, lax.shift_right_logical(row, 3) * 4 + low, -1)
        gate = jnp.zeros((ndev * 8, tok), F32)
        for j in range(ids_ref.shape[0]):
            gate = gate + jnp.where(ids_ref[j : j + 1, :] == expert, gates_ref[j : j + 1, :], 0.0)
        dense[...] = gate

        @pl.loop(0, ndev, unroll=4)
        def _(d):
            g = dense[pl.ds(pl.multiple_of(d * 8, 8), 8), :]
            hi = g.astype(BF16).astype(F32)
            mid = (g - hi).astype(BF16).astype(F32)
            low = g - hi - mid
            parts = jnp.concatenate([hi, mid, low, jnp.zeros_like(g)], axis=0).astype(BF16)
            slot = slot_ref[lax.div(d, nq), pl.ds(lax.rem(d, nq), 1), :]
            spot = lax.broadcasted_iota(jnp.int32, (128, tok), 0) == slot
            spot = jnp.where(spot, 1.0, 0.0).astype(BF16)
            got = lax.dot_general(parts, spot, (((1,), (1,)), ((), ())), preferred_element_type=F32)
            sgate_ref[d] = got[0:8] + got[8:16] + got[16:24]

    def run(word):
        what, s, h = word[0], int(word[1]), int(word[2])
        if what == "p":
            pick(s, h)
        if what == "X":
            send_picked(s, h, (1, 2, 3))
        if what == "G":
            send_picked(s, h, (6, 7))
        if what == "Y":
            send_picked(s, h, (4, 5))
        if what == "x":
            send_back(s, h, (1, 2, 3))
        if what == "g":
            send_back(s, h, (6, 7))
        if what == "y":
            send_back(s, h, (4, 5))
        if what == "u":
            pass_on(s, h)

    before, seen = {}, 0
    for word in ORDER:
        if word[0] == "c":
            seen += 1
        else:
            before.setdefault(seen, []).append(word)

    barrier = pltpu.get_barrier_semaphore()
    for o in range(1, ndev):
        d = lax.rem(me + o, ndev)
        pl.semaphore_signal(barrier, inc=1, device_id=at(lax.div(d, nq), lax.rem(d, nq)), device_id_type=MESH)
    load_x = pltpu.make_async_copy(x_ref, xall.at[z], x_sem)
    load_x.start()
    for c in weight_copies(0, 0):
        c.start()
    slot_table()
    smap[z] = slot_ref[z]
    load_x.wait()
    run(ORDER[0])
    pl.semaphore_wait(barrier, ndev - 1)
    for o in range(1, nz):
        slot_copy(o).start()
    for h in range(2):
        @pl.when(z > 0)
        def _():
            z_rows(z, z - 1, 0, h).start()

        @pl.when(z < nz - 1)
        def _():
            z_rows(z, z + 1, 1, h).start()

    gates_sent = False
    for word in before.get(0, ())[1:]:
        if word[:2] == "p1" and not gates_sent:
            gates_sent = True
            gate_table()
            for o in range(1, ndev):
                gate_copy(o).start()
            grecv[me] = sgate_ref[me]
        run(word)
    for o in range(1, ndev):
        s = lax.rem(me + o, ndev)
        rcopy(sgate_ref.at[0], grecv.at[s], g_send.at[o], g_recv.at[s], at(z, q)).wait_recv()

    def expert_step(i, _):
        s, e, slot = lax.div(i, 4), lax.rem(i, 4), lax.rem(i, 2)
        k = plane_of(s)

        for n in range(1, 16):
            if n in before:
                @pl.when(i == n)
                def _():
                    for word in before[n]:
                        run(word)

        @pl.when(i < 15)
        def _():
            for c in weight_copies(lax.rem(i + 1, 4), 1 - slot):
                c.start()

        @pl.when(e == 0)
        def _():
            d_wait(k)
            by_slot = grecv[pl.ds(k * nq, nq)].reshape(nq * 8, 128).T
            for r in range(nq):
                for j in range(4):
                    one = by_slot[0:cap, r * 8 + j : r * 8 + j + 1]
                    gb[j, r * cap : (r + 1) * cap, :] = jnp.broadcast_to(one, (cap, 128))

        for c in weight_copies(e, slot):
            c.wait()

        @pl.loop(0, ff // ft, unroll=3)
        def _(n):
            cols = pl.ds(pl.multiple_of(n * ft, ft), ft)
            xin = drecv[k].reshape(rows, hid)
            a = jnp.dot(xin, wb1[slot, :, cols], preferred_element_type=F32)
            b = jnp.dot(xin, wb3[slot, :, cols], preferred_element_type=F32)
            hbuf[:, cols] = (a * jax.nn.sigmoid(a) * b).astype(BF16)

        @pl.loop(0, hid // ot, unroll=8)
        def _(n):
            cols = pl.ds(pl.multiple_of(n * ot, ot), ot)
            o = jnp.dot(hbuf[...], wb2[slot, :, cols], preferred_element_type=F32)
            g = jnp.concatenate([gb[e]] * (ot // 128), axis=1)
            term = jnp.where(g > 0.0, o * g, 0.0)
            acc[:, cols] = jnp.where(e == 0, 0.0, acc[:, cols]) + term

        @pl.when(e == 3)
        def _():
            @pl.loop(0, hid // nt)
            def _(n):
                cols = pl.ds(pl.multiple_of(n * nt, nt), nt)
                drecv[k, :, :, cols] = acc[:, cols].astype(BF16).reshape(nq, cap, nt)

        return 0

    lax.fori_loop(0, 16, expert_step, 0)
    for word in before.get(16, ()):
        run(word)

    for h in range(2):
        @pl.when(z > 0)
        def _():
            z_rows(z, z - 1, 0, h).wait_send()

        @pl.when(z < nz - 1)
        def _():
            z_rows(z, z + 1, 1, h).wait_send()

        for s in range(1, 4):
            zr_copy(chunk[s], h, s, z, k1).wait_send()
        for f in range(1, nq):
            for s in range(4):
                r_copy(s, h, f).wait_send()
                if s >= 2:
                    d_copy(s, h, f).wait_send()
    for o in range(1, nz):
        slot_copy(o).wait_send()
    for o in range(1, ndev):
        gate_copy(o).wait_send()


def moe_call(dims, x, ids, gates, w1, w3, w2, capacity):
    nz, ny, nx = dims
    nq = ny * nx
    ndev = nz * nq
    tok, hid = x.shape
    ff = w1.shape[2]
    dma = pltpu.SemaphoreType.DMA
    vmem = pl.BlockSpec(memory_space=pltpu.VMEM)
    hbm = pl.BlockSpec(memory_space=pl.ANY)
    return pl.pallas_call(
        functools.partial(moe_kernel, dims),
        out_shape=jax.ShapeDtypeStruct((tok, hid), BF16),
        in_specs=[hbm, vmem, vmem, hbm, hbm, hbm],
        out_specs=vmem,
        scratch_shapes=[
            pltpu.VMEM((nz, nq, tok), jnp.int32),
            pltpu.VMEM((ndev, 8, 128), F32),
            pltpu.VMEM((ndev * 8, tok), F32),
            pltpu.VMEM((nz, tok, hid), BF16),
            pltpu.VMEM((nz, nq, tok), jnp.int32),
            pltpu.VMEM((ndev, 8, 128), F32),
            pltpu.VMEM((nz, nq * capacity, tok), BF16),
            pltpu.VMEM((2, nq, capacity, hid), BF16),
            pltpu.VMEM((nz, nq, capacity, hid), BF16),
            pltpu.VMEM((nz, nq, capacity, hid), BF16),
            pltpu.VMEM((nz, tok, hid), BF16),
            pltpu.VMEM((nq * capacity, hid), F32),
            pltpu.VMEM((nq * capacity, ff), BF16),
            pltpu.VMEM((4, nq * capacity, 128), F32),
            pltpu.VMEM((2, hid, ff), BF16),
            pltpu.VMEM((2, hid, ff), BF16),
            pltpu.VMEM((2, ff, hid), BF16),
            dma,
            dma((2, 3)),
            dma((5, 2)),
            dma((nz, 2)),
            dma((nz,)),
            dma((nz,)),
            dma((ndev,)),
            dma((ndev,)),
            dma((4, nq)),
            dma((2 * nz, nq)),
            dma((2 * nz, nq)),
            dma((2 * nz, nq)),
            dma((nz, 2)),
            dma((nz, 2)),
        ],
        compiler_params=pltpu.CompilerParams(collective_id=0, has_side_effects=True, vmem_limit_bytes=66 * 1000 * 1000),
    )(x, ids, gates, w1, w3, w2)


def solution(mesh):
    ep_axes = tuple(mesh.axis_names)
    dims = tuple(mesh.shape[axis_name] for axis_name in ep_axes)
    num_devices = math.prod(dims)
    row_spec = P(ep_axes, None)
    w_spec = P(ep_axes, None, None)

    def local_layer(tokens, expert_ids, gate_weights, w_gate, w_up, w_down):
        tok_dev = tokens.shape[0]
        top_k = expert_ids.shape[1]
        capacity = tok_dev * top_k // num_devices
        return moe_call(dims, tokens, expert_ids.T, gate_weights.T, w_gate, w_up, w_down, capacity)

    return jax.shard_map(local_layer, mesh=mesh, in_specs=(row_spec, row_spec, row_spec, w_spec, w_spec, w_spec), out_specs=row_spec, check_vma=False)
```

```python
import functools
import math

import jax
import jax.numpy as jnp
from jax import lax
from jax.experimental import pallas as pl
from jax.experimental.pallas import tpu as pltpu
from jax.sharding import PartitionSpec as P

MESH = pl.DeviceIdType.MESH
F32 = jnp.float32
BF16 = jnp.bfloat16


ORDER = (
    "e00", "e01", "p00", "p01", "e10", "e11", "c00", "p10", "c01", "e20", "p11", "c02", "c03", "e21", "p20", "c10",
    "e30", "p21", "c11", "c12", "e31", "c13", "b11", "c20", "p31", "c21", "p30", "n11", "c22", "c23", "b10", "b20",
    "c30", "c31", "b21", "c32", "n20", "u11", "c33", "b31", "b30", "u20", "n31", "b00", "n30", "n10", "n21", "u31",
    "u30", "b01", "n00", "u21", "u10", "n01", "u00", "u01",
)
LAST = ((0, 1, 4, 5), (0, 1, 2, 3))
SWAP = (2, 4)


def moe_kernel(
    dims, x_ref, ids_ref, gates_ref, w1_ref, w3_ref, w2_ref, out_ref,
    slot_ref, sgate_ref, dense, xall, xnb, smap, grecv, place, sbuf, drecv, rrecv, prcv, zret, acc, hbuf, gb, wb1, wb3, wb2,
    x_sem, w_sem, zs_send, zs_recv, sm_send, sm_recv, g_send, g_recv, e_send, e_recv, d_send, d_recv, r_send, r_recv,
    p_send, p_recv, zr_send, zr_recv,
):
    nz, ny, nx = dims
    nq = ny * nx
    ndev = nz * nq
    tok, hid = xall.shape[1:]
    cap = sbuf.shape[3]
    ff = wb1.shape[2]
    rows = nq * cap
    nt = 256
    ft = 256
    ot = 256
    quarter = hid // 4
    z = lax.axis_index("ez")
    iy, ix = lax.axis_index("ey"), lax.axis_index("ex")
    q = iy * nx + ix
    me = z * nq + q
    col, core = lax.div(ix, 2), lax.rem(ix, 2)

    def at(zz, qq):
        return (zz, lax.div(qq, nx), lax.rem(qq, nx))

    def rcopy(src, dst, ss, rs, dev):
        return pltpu.make_async_remote_copy(src_ref=src, dst_ref=dst, send_sem=ss, recv_sem=rs, device_id=dev, device_id_type=MESH)

    inner = lax.div(z * (3 - z), 2)
    flip = lax.div(z, 2)

    def mirrored(b):
        return b + flip * (3 - 2 * b)

    k1, k2, k3 = mirrored(1 - inner), mirrored(2), mirrored(3)
    chunk = (z, k1, k2, k3)

    def plane_of(s):
        return (
            z * lax.div(3 - s, 3)
            + k1 * (lax.rem(s, 2) * lax.div(4 - s, 3))
            + k2 * ((1 - lax.rem(s, 2)) * lax.div(s, 2))
            + k3 * lax.div(s, 3)
        )

    def peer(f):
        fy, fx, fc = f // 4, (f // 2) % 2, f % 2
        return (iy + fy * (1 - 2 * iy)) * nx + (col + fx * (1 - 2 * col)) * 2 + core + fc * (1 - 2 * core)

    def part(h, g):
        return pl.ds((2 * g + h) * quarter, quarter)

    def tiles(h, g, body):
        @pl.loop(0, quarter // nt)
        def _(n):
            body(pl.ds(pl.multiple_of((2 * g + h) * quarter + n * nt, nt), nt))

    def weight_copies(e, slot):
        return (
            pltpu.make_async_copy(w1_ref.at[e], wb1.at[slot], w_sem.at[slot, 0]),
            pltpu.make_async_copy(w3_ref.at[e], wb3.at[slot], w_sem.at[slot, 1]),
        )

    def down_copy(e):
        return pltpu.make_async_copy(w2_ref.at[e], wb2, w_sem.at[0, 2])

    def z_rows(k, dst_z, n, h, g):
        ref = xall.at[k, :, part(h, g)]
        return rcopy(ref, ref, zs_send.at[n, h], zs_recv.at[k, h], at(dst_z, q))

    def pair(ref, ss, rs):
        both = ref.at[0, :, pl.ds(0, 2 * quarter)]
        return rcopy(both, both, ss, rs, at(z, q))

    def z_wait(k, h):
        pair(xall, zs_send.at[0, h], zs_recv.at[k, h]).wait_recv()

    def z_sent(n, h):
        pair(xall, zs_send.at[n, h], zs_recv.at[0, h]).wait_send()

    def blocks(n, ss, rs):
        ref = drecv.at[0, pl.ds(0, n), :, pl.ds(0, 2 * quarter)]
        return rcopy(ref, ref, ss, rs, at(z, q))

    def tables(ref, n, ss, rs):
        ref = ref.at[pl.ds(0, n)]
        return rcopy(ref, ref, ss, rs, at(z, q))

    def slot_copy(o, role):
        dz = lax.rem(z + o, nz)
        return rcopy(slot_ref.at[dz], smap.at[z, role], sm_send, sm_recv.at[z], at(dz, peer((0, 2, 4)[role])))

    def gate_copy(o):
        d = lax.rem(me + o, ndev)
        return rcopy(sgate_ref.at[d], grecv.at[me], g_send, g_recv, at(lax.div(d, nq), lax.rem(d, nq)))

    def source(f, g, src):
        return peer(f ^ (SWAP[g] * src))

    def e_copy(s, h, g):
        k = chunk[s]
        return rcopy(xall.at[k, :, part(h, g)], xnb.at[k, :, part(h, g)], e_send.at[s, h], e_recv.at[k, h], at(z, peer(SWAP[g])))

    def d_copy(s, h, g, src, i):
        k = chunk[s]
        to = drecv.at[k, source(0, g, src), :, part(h, g)]
        return rcopy(sbuf.at[s % 2, src, i, :, part(h, g)], to, d_send.at[s % 2, h], d_recv.at[k, h], at(z, peer(LAST[g][i])))

    def r_copy(s, h, g, src, i):
        k, f = chunk[s], LAST[g][i]
        to = rrecv.at[k, src, i, :, part(h, g)]
        return rcopy(drecv.at[k, source(f, g, src), :, part(h, g)], to, r_send.at[s, h], r_recv.at[k, 2 * h + src], at(z, peer(f)))

    def p_copy(s, h, g):
        k = chunk[s]
        return rcopy(xnb.at[k, :, part(h, g)], prcv.at[k, :, part(h, g)], p_send.at[s, h], p_recv.at[k, h], at(z, peer(SWAP[g])))

    def zr_copy(k, h, g, n, slot, dst_z):
        to = zret.at[slot, :, part(h, g)]
        return rcopy(xall.at[k, :, part(h, g)], to, zr_send.at[n, h], zr_recv.at[slot, h], at(dst_z, q))

    def zr_wait(slot, h):
        pair(zret, zr_send.at[0, h], zr_recv.at[slot, h]).wait_recv()

    def summed(k, g, src, cols):
        got = rrecv[k, src, :, :, cols].reshape(4 * cap, nt)
        return lax.dot_general(place[k, 2 * g + src], got, (((0,), (0,)), ((), ())), preferred_element_type=F32)

    def swap_rows(s, h):
        k = chunk[s]
        if s == 1:
            z_wait(k1, h)
        if s >= 1:
            @pl.when(inner == 1)
            def _():
                if s == 1:
                    z_wait(k2, h)
                    for g in range(2):
                        z_rows(k1, k2, 2, h, g).start()
                        z_rows(k2, k1, 3, h, g).start()
                if s == 2:
                    z_wait(k3, h)
                    for g in range(2):
                        z_rows(k3, k1, 4, h, g).start()

        if s >= 2:
            @pl.when(inner == 0)
            def _():
                z_wait(k, h)
        for g in range(2):
            e_copy(s, h, g).start()

    placed = set()

    def pick(s, h):
        k = chunk[s]
        pair(xnb, e_send.at[s, h], e_recv.at[k, h]).wait_recv()
        if s >= 2:
            blocks(6, d_send.at[s % 2, h], d_recv.at[k, h]).wait_send()
        if s not in placed:
            placed.add(s)
            tables(smap.at[k], 3 if s else 2, sm_send, sm_recv.at[k]).wait_recv()
            lane_slot = lax.broadcasted_iota(jnp.int32, (cap, tok), 0)
            for g in range(2):
                for src in range(2):
                    for i in range(4):
                        hit = lane_slot == smap[k, src * (1 + g), pl.ds(peer(LAST[g][i]), 1), :]
                        place[k, 2 * g + src, i * cap : (i + 1) * cap, :] = jnp.where(hit, 1.0, 0.0).astype(BF16)
        for g in range(2):
            for src in range(2):
                rows_of = xnb if src else xall

                def tile(cols, g=g, src=src, rows_of=rows_of):
                    got = jnp.dot(place[k, 2 * g + src], rows_of[k, :, cols], preferred_element_type=F32).astype(BF16)
                    sbuf[s % 2, src, :, :, cols] = got.reshape(4, cap, nt)
                    drecv[k, source(0, g, src), :, cols] = sbuf[s % 2, src, 0, :, cols]

                tiles(h, g, tile)
                for i in range(1, 4):
                    d_copy(s, h, g, src, i).start()

    def d_wait(k):
        for h in range(2):
            blocks(6, d_send.at[0, h], d_recv.at[k, h]).wait_recv()

    def send_back(s, h):
        k = chunk[s]
        for src in (1, 0):
            for i in range(1, 4):
                for g in range(2):
                    r_copy(s, h, g, src, i).start()
        for g in range(2):
            def tile(cols, g=g):
                for src in range(2):
                    rrecv[k, src, 0, :, cols] = drecv[k, source(0, g, src), :, cols]

            tiles(h, g, tile)

    def r_wait(s, h, src):
        k = chunk[s]
        blocks(3, r_send.at[s, h], r_recv.at[k, 2 * h + src]).wait_recv()

    def sum_neighbour(s, h):
        k = chunk[s]
        r_wait(s, h, 1)
        for g in range(2):
            def tile(cols, g=g):
                xnb[k, :, cols] = summed(k, g, 1, cols).astype(BF16)

            tiles(h, g, tile)
            p_copy(s, h, g).start()

    def pass_on(s, h):
        k = chunk[s]
        r_wait(s, h, 0)
        pair(prcv, p_send.at[s, h], p_recv.at[k, h]).wait_recv()

        def own(g, cols):
            return summed(k, g, 0, cols) + prcv[k, :, cols].astype(F32)

        if s == 0:
            zr_wait(k1, h)
            zr_wait(k2, h)
            for g in range(2):
                def tile(cols, g=g):
                    total = own(g, cols) + xall[k, :, cols].astype(F32)
                    total = total + zret[k1, :, cols].astype(F32) + zret[k2, :, cols].astype(F32)
                    out_ref[:, cols] = total.astype(BF16)

                tiles(h, g, tile)
            return

        pair(xall, e_send.at[s, h], e_recv.at[k, h]).wait_send()

        @pl.when(inner == 1)
        def _():
            z_sent(s + 1, h)

        def plain():
            for g in range(2):
                def tile(cols, g=g):
                    xall[k, :, cols] = own(g, cols).astype(BF16)

                tiles(h, g, tile)

        if s == 1:
            plain()
            for g in range(2):
                zr_copy(k, h, g, s, z, k).start()
            return
        slot = z if s == 2 else k

        @pl.when(inner == 1)
        def _():
            zr_wait(slot, h)
            for g in range(2):
                def tile(cols, g=g):
                    xall[k, :, cols] = (own(g, cols) + zret[slot, :, cols].astype(F32)).astype(BF16)

                tiles(h, g, tile)
                zr_copy(k, h, g, s, z, k).start()

        @pl.when(inner == 0)
        def _():
            plain()
            for g in range(2):
                zr_copy(k, h, g, s, k1 if s == 2 else k, k1).start()

    def slot_table():
        device = lax.broadcasted_iota(jnp.int32, (ndev, tok), 0)
        hit = None
        for j in range(ids_ref.shape[0]):
            here = lax.shift_right_logical(ids_ref[j : j + 1, :], 2) == device
            hit = here if hit is None else jnp.logical_or(hit, here)
        hit = jnp.where(hit, 1.0, 0.0)
        upto = lax.broadcasted_iota(jnp.int32, (tok, tok), 0) <= lax.broadcasted_iota(jnp.int32, (tok, tok), 1)
        upto = jnp.where(upto, 1.0, 0.0).astype(BF16)
        count = jnp.dot(hit.astype(BF16), upto, preferred_element_type=F32)
        slot = jnp.where(hit > 0.0, count - 1.0, -1.0).astype(jnp.int32)
        slot_ref[...] = slot.reshape(nz, nq, tok)

    def gate_table():
        row = lax.broadcasted_iota(jnp.int32, (ndev * 8, tok), 0)
        low = jnp.bitwise_and(row, 7)
        expert = jnp.where(low < 4, lax.shift_right_logical(row, 3) * 4 + low, -1)
        gate = jnp.zeros((ndev * 8, tok), F32)
        for j in range(ids_ref.shape[0]):
            gate = gate + jnp.where(ids_ref[j : j + 1, :] == expert, gates_ref[j : j + 1, :], 0.0)
        dense[...] = gate

        @pl.loop(0, ndev, unroll=4)
        def _(d):
            g = dense[pl.ds(pl.multiple_of(d * 8, 8), 8), :]
            hi = g.astype(BF16).astype(F32)
            mid = (g - hi).astype(BF16).astype(F32)
            low = g - hi - mid
            parts = jnp.concatenate([hi, mid, low, jnp.zeros_like(g)], axis=0).astype(BF16)
            slot = slot_ref[lax.div(d, nq), pl.ds(lax.rem(d, nq), 1), :]
            spot = lax.broadcasted_iota(jnp.int32, (128, tok), 0) == slot
            spot = jnp.where(spot, 1.0, 0.0).astype(BF16)
            got = lax.dot_general(parts, spot, (((1,), (1,)), ((), ())), preferred_element_type=F32)
            sgate_ref[d] = got[0:8] + got[8:16] + got[16:24]

    steps = {"e": swap_rows, "p": pick, "b": send_back, "n": sum_neighbour, "u": pass_on}

    def run(word):
        steps[word[0]](int(word[1]), int(word[2]))

    before, seen = {}, 0
    for word in ORDER:
        if word[0] == "c":
            seen += 1
        else:
            before.setdefault(seen, []).append(word)

    barrier = pltpu.get_barrier_semaphore()

    @pl.loop(1, ndev)
    def _(o):
        d = lax.rem(me + o, ndev)
        pl.semaphore_signal(barrier, inc=1, device_id=at(lax.div(d, nq), lax.rem(d, nq)), device_id_type=MESH)

    load_x = pltpu.make_async_copy(x_ref, xall.at[z], x_sem)
    load_x.start()
    for c in weight_copies(0, 0):
        c.start()
    slot_table()
    smap[z, 0] = slot_ref[z]
    load_x.wait()
    pl.semaphore_wait(barrier, ndev - 1)
    for h in range(2):
        for g in range(2):
            @pl.when(z > 0)
            def _():
                z_rows(z, z - 1, 0, h, g).start()

            @pl.when(z < nz - 1)
            def _():
                z_rows(z, z + 1, 1, h, g).start()

        swap_rows(0, h)
        for o in range(nz):
            for role in range(3):
                if h == 0 and (o or role):
                    slot_copy(o, role).start()
    gate_table()

    @pl.loop(1, ndev)
    def _(o):
        gate_copy(o).start()

    grecv[me] = sgate_ref[me]
    for word in before.get(0, ())[2:]:
        run(word)
    tables(grecv, ndev - 1, g_send, g_recv).wait_recv()

    def expert_step(i, _):
        s, e, slot = lax.div(i, 4), lax.rem(i, 4), lax.rem(i, 2)
        k = plane_of(s)

        for n in range(1, 16):
            if n in before:
                @pl.when(i == n)
                def _():
                    for word in before[n]:
                        run(word)

        down_copy(e).start()

        @pl.when(i < 15)
        def _():
            for c in weight_copies(lax.rem(i + 1, 4), 1 - slot):
                c.start()

        @pl.when(e == 0)
        def _():
            d_wait(k)
            by_slot = grecv[pl.ds(k * nq, nq)].reshape(nq * 8, 128).T
            for r in range(nq):
                for j in range(4):
                    one = by_slot[0:cap, r * 8 + j : r * 8 + j + 1]
                    gb[j, r * cap : (r + 1) * cap, :] = jnp.broadcast_to(one, (cap, 128))

        for c in weight_copies(e, slot):
            c.wait()

        @pl.loop(0, ff // ft, unroll=3)
        def _(n):
            cols = pl.ds(pl.multiple_of(n * ft, ft), ft)
            xin = drecv[k].reshape(rows, hid)
            a = jnp.dot(xin, wb1[slot, :, cols], preferred_element_type=F32)
            b = jnp.dot(xin, wb3[slot, :, cols], preferred_element_type=F32)
            hbuf[:, cols] = (a * jax.nn.sigmoid(a) * b).astype(BF16)

        down_copy(e).wait()

        @pl.loop(0, hid // ot, unroll=8)
        def _(n):
            cols = pl.ds(pl.multiple_of(n * ot, ot), ot)
            o = jnp.dot(hbuf[...], wb2[:, cols], preferred_element_type=F32)
            g = jnp.concatenate([gb[e]] * (ot // 128), axis=1)
            term = jnp.where(g > 0.0, o * g, 0.0)
            acc[:, cols] = jnp.where(e == 0, 0.0, acc[:, cols]) + term

        @pl.when(e == 3)
        def _():
            @pl.loop(0, hid // nt)
            def _(n):
                cols = pl.ds(pl.multiple_of(n * nt, nt), nt)
                drecv[k, :, :, cols] = acc[:, cols].astype(BF16).reshape(nq, cap, nt)

        return 0

    lax.fori_loop(0, 16, expert_step, 0)
    for word in before.get(16, ()):
        run(word)

    for h in range(2):
        @pl.when(z > 0)
        def _():
            z_sent(0, h)

        @pl.when(z < nz - 1)
        def _():
            z_sent(1, h)

        pair(xall, e_send.at[0, h], e_recv.at[0, h]).wait_send()
        for s in range(4):
            pair(xnb, p_send.at[s, h], p_recv.at[0, h]).wait_send()
            if s:
                pair(xall, zr_send.at[s, h], zr_recv.at[0, h]).wait_send()
            if s >= 2:
                blocks(6, d_send.at[s % 2, h], d_recv.at[0, h]).wait_send()
            blocks(6, r_send.at[s, h], r_recv.at[0, h]).wait_send()
    tables(sgate_ref, ndev - 1, g_send, g_recv).wait_send()
    tables(sgate_ref, 2 * (3 * nz - 1), sm_send, sm_recv.at[0]).wait_send()


def moe_call(dims, x, ids, gates, w1, w3, w2, capacity):
    nz, ny, nx = dims
    nq = ny * nx
    ndev = nz * nq
    tok, hid = x.shape
    ff = w1.shape[2]
    dma = pltpu.SemaphoreType.DMA
    vmem = pl.BlockSpec(memory_space=pltpu.VMEM)
    hbm = pl.BlockSpec(memory_space=pl.ANY)
    return pl.pallas_call(
        functools.partial(moe_kernel, dims),
        out_shape=jax.ShapeDtypeStruct((tok, hid), BF16),
        in_specs=[hbm, vmem, vmem, hbm, hbm, hbm],
        out_specs=vmem,
        scratch_shapes=[
            pltpu.VMEM((nz, nq, tok), jnp.int32),
            pltpu.VMEM((ndev, 8, 128), F32),
            pltpu.VMEM((ndev * 8, tok), F32),
            pltpu.VMEM((nz, tok, hid), BF16),
            pltpu.VMEM((nz, tok, hid), BF16),
            pltpu.VMEM((nz, 3, nq, tok), jnp.int32),
            pltpu.VMEM((ndev, 8, 128), F32),
            pltpu.VMEM((nz, 4, 4 * capacity, tok), BF16),
            pltpu.VMEM((2, 2, 4, capacity, hid), BF16),
            pltpu.VMEM((nz, nq, capacity, hid), BF16),
            pltpu.VMEM((nz, 2, 4, capacity, hid), BF16),
            pltpu.VMEM((nz, tok, hid), BF16),
            pltpu.VMEM((nz, tok, hid), BF16),
            pltpu.VMEM((nq * capacity, hid), F32),
            pltpu.VMEM((nq * capacity, ff), BF16),
            pltpu.VMEM((4, nq * capacity, 128), F32),
            pltpu.VMEM((2, hid, ff), BF16),
            pltpu.VMEM((2, hid, ff), BF16),
            pltpu.VMEM((ff, hid), BF16),
            dma,
            dma((2, 3)),
            dma((5, 2)),
            dma((nz, 2)),
            dma,
            dma((nz,)),
            dma,
            dma,
            dma((nz, 2)),
            dma((nz, 2)),
            dma((2, 2)),
            dma((nz, 2)),
            dma((nz, 2)),
            dma((nz, 4)),
            dma((nz, 2)),
            dma((nz, 2)),
            dma((nz, 2)),
            dma((nz, 2)),
        ],
        compiler_params=pltpu.CompilerParams(collective_id=0, has_side_effects=True, vmem_limit_bytes=67 * 1000 * 1000),
    )(x, ids, gates, w1, w3, w2)


def solution(mesh):
    ep_axes = tuple(mesh.axis_names)
    dims = tuple(mesh.shape[axis_name] for axis_name in ep_axes)
    num_devices = math.prod(dims)
    row_spec = P(ep_axes, None)
    w_spec = P(ep_axes, None, None)

    def local_layer(tokens, expert_ids, gate_weights, w_gate, w_up, w_down):
        tok_dev = tokens.shape[0]
        top_k = expert_ids.shape[1]
        capacity = tok_dev * top_k // num_devices
        return moe_call(dims, tokens, expert_ids.T, gate_weights.T, w_gate, w_up, w_down, capacity)

    return jax.shard_map(local_layer, mesh=mesh, in_specs=(row_spec, row_spec, row_spec, w_spec, w_spec, w_spec), out_specs=row_spec, check_vma=False)
```

```python
import functools
import math

import jax
import jax.numpy as jnp
from jax import lax
from jax.experimental import pallas as pl
from jax.experimental.pallas import tpu as pltpu
from jax.sharding import PartitionSpec as P

MESH = pl.DeviceIdType.MESH
F32 = jnp.float32
BF16 = jnp.bfloat16


ORDER = (
    "e00", "e01", "p00", "p01", "e10", "e11", "c00", "p10", "c01", "p11", "e20", "c02", "c03", "e21", "c10", "p20",
    "c11", "p21", "c12", "e30", "c13", "e31", "c20", "b11", "p30", "c21", "p31", "c22", "n11", "c23", "b20", "b01",
    "c30", "c31", "u11", "n20", "c32", "c33", "b31", "b30", "u20", "n31", "b21", "n30", "u31", "b10", "n21", "u30",
    "n10", "b00", "u21", "n01", "u10", "n00", "u01", "u00",
)
LAST = ((0, 1, 4, 5), (0, 1, 2, 3))
SWAP = (2, 4)


def moe_kernel(
    dims, x_ref, ids_ref, gates_ref, w1_ref, w3_ref, w2_ref, out_ref,
    slot_ref, sgate_ref, xall, xnb, smap, grecv, place, sbuf, drecv, rrecv, prcv, zret, acc, hbuf, gb, wb1, wb3, wb2,
    x_sem, w_sem, zs_send, zs_recv, sm_send, sm_recv, g_send, g_recv, e_send, e_recv, d_send, d_recv, r_send, r_recv,
    p_send, p_recv, zr_send, zr_recv,
):
    nz, ny, nx = dims
    nq = ny * nx
    ndev = nz * nq
    tok, hid = xall.shape[1:]
    cap = sbuf.shape[2]
    ff = wb1.shape[2]
    rows = nq * cap
    nt = 256
    ft = 256
    ot = 256
    quarter = hid // 4
    z = lax.axis_index("ez")
    iy, ix = lax.axis_index("ey"), lax.axis_index("ex")
    q = iy * nx + ix
    me = z * nq + q
    col, core = lax.div(ix, 2), lax.rem(ix, 2)

    def at(zz, qq):
        return (zz, lax.div(qq, nx), lax.rem(qq, nx))

    def rcopy(src, dst, ss, rs, dev):
        return pltpu.make_async_remote_copy(src_ref=src, dst_ref=dst, send_sem=ss, recv_sem=rs, device_id=dev, device_id_type=MESH)

    inner = lax.div(z * (3 - z), 2)
    flip = lax.div(z, 2)

    def mirrored(b):
        return b + flip * (3 - 2 * b)

    k1, k2, k3 = mirrored(1 - inner), mirrored(2), mirrored(3)
    chunk = (z, k1, k2, k3)

    def plane_of(s):
        return (
            z * lax.div(3 - s, 3)
            + k1 * (lax.rem(s, 2) * lax.div(4 - s, 3))
            + k2 * ((1 - lax.rem(s, 2)) * lax.div(s, 2))
            + k3 * lax.div(s, 3)
        )

    def peer(f):
        fy, fx, fc = f // 4, (f // 2) % 2, f % 2
        return (iy + fy * (1 - 2 * iy)) * nx + (col + fx * (1 - 2 * col)) * 2 + core + fc * (1 - 2 * core)

    def part(h, g):
        return pl.ds((2 * g + h) * quarter, quarter)

    def tiles(h, g, body):
        body(part(h, g))

    def weight_copies(e, slot):
        return (
            pltpu.make_async_copy(w1_ref.at[e], wb1.at[slot], w_sem.at[slot, 0]),
            pltpu.make_async_copy(w3_ref.at[e], wb3.at[slot], w_sem.at[slot, 1]),
        )

    def down_copy(e):
        return pltpu.make_async_copy(w2_ref.at[e], wb2, w_sem.at[0, 2])

    def z_rows(k, dst_z, n, h, g):
        ref = xall.at[k, :, part(h, g)]
        return rcopy(ref, ref, zs_send.at[n, h], zs_recv.at[k, h], at(dst_z, q))

    def pair(ref, ss, rs):
        both = ref.at[0, :, pl.ds(0, 2 * quarter)]
        return rcopy(both, both, ss, rs, at(z, q))

    def z_wait(k, h):
        pair(xall, zs_send.at[0, h], zs_recv.at[k, h]).wait_recv()

    def z_sent(n, h):
        pair(xall, zs_send.at[n, h], zs_recv.at[0, h]).wait_send()

    def blocks(n, ss, rs):
        ref = drecv.at[0, pl.ds(0, n), :, pl.ds(0, 2 * quarter)]
        return rcopy(ref, ref, ss, rs, at(z, q))

    def tables(ref, n, ss, rs):
        ref = ref.at[pl.ds(0, n)]
        return rcopy(ref, ref, ss, rs, at(z, q))

    def slot_copy(o, role):
        dz = lax.rem(z + o, nz)
        return rcopy(slot_ref.at[dz], smap.at[z, role], sm_send, sm_recv.at[z], at(dz, peer((0, 2, 4)[role])))

    def gate_copy(o):
        d = lax.rem(me + o, ndev)
        return rcopy(sgate_ref.at[d], grecv.at[me], g_send, g_recv, at(lax.div(d, nq), lax.rem(d, nq)))

    def source(f, g, src):
        return peer(f ^ (SWAP[g] * src))

    def e_copy(s, h, g):
        k = chunk[s]
        return rcopy(xall.at[k, :, part(h, g)], xnb.at[k, :, part(h, g)], e_send.at[s, h], e_recv.at[k, h], at(z, peer(SWAP[g])))

    def d_copy(s, h, g, src, i):
        k = chunk[s]
        to = drecv.at[k, source(0, g, src), :, part(h, g)]
        return rcopy(sbuf.at[src, i, :, part(h, g)], to, d_send.at[h], d_recv.at[k, h], at(z, peer(LAST[g][i])))

    def r_copy(s, h, g, src, i):
        k, f = chunk[s], LAST[g][i]
        to = rrecv.at[k, src, i, :, part(h, g)]
        return rcopy(drecv.at[k, source(f, g, src), :, part(h, g)], to, r_send.at[s, h], r_recv.at[k, 2 * h + src], at(z, peer(f)))

    def p_copy(s, h, g):
        k = chunk[s]
        return rcopy(xnb.at[k, :, part(h, g)], prcv.at[k, :, part(h, g)], p_send.at[s, h], p_recv.at[k, h], at(z, peer(SWAP[g])))

    def zr_copy(k, h, g, n, slot, dst_z):
        to = zret.at[slot, :, part(h, g)]
        return rcopy(xall.at[k, :, part(h, g)], to, zr_send.at[n, h], zr_recv.at[slot, h], at(dst_z, q))

    def zr_wait(slot, h):
        pair(zret, zr_send.at[0, h], zr_recv.at[slot, h]).wait_recv()

    def summed(k, g, src, cols):
        got = rrecv[k, src, :, :, cols].reshape(4 * cap, quarter)
        return lax.dot_general(place[k, 2 * g + src], got, (((0,), (0,)), ((), ())), preferred_element_type=F32)

    def swap_rows(s, h):
        k = chunk[s]
        if s == 1:
            z_wait(k1, h)
        if s >= 1:
            @pl.when(inner == 1)
            def _():
                if s == 1:
                    z_wait(k2, h)
                    for g in range(2):
                        z_rows(k1, k2, 2, h, g).start()
                        z_rows(k2, k1, 3, h, g).start()
                if s == 2:
                    z_wait(k3, h)
                    for g in range(2):
                        z_rows(k3, k1, 4, h, g).start()

        if s >= 2:
            @pl.when(inner == 0)
            def _():
                z_wait(k, h)
        for g in range(2):
            e_copy(s, h, g).start()

    placed = set()

    def pick(s, h):
        k = chunk[s]
        pair(xnb, e_send.at[s, h], e_recv.at[k, h]).wait_recv()
        if s >= 1:
            blocks(6, d_send.at[h], d_recv.at[k, h]).wait_send()
        if s not in placed:
            placed.add(s)
            tables(smap.at[k], 3 if s else 2, sm_send, sm_recv.at[k]).wait_recv()
            lane_slot = lax.broadcasted_iota(jnp.int32, (cap, tok), 0)
            for g in range(2):
                for src in range(2):
                    for i in range(4):
                        hit = lane_slot == smap[k, src * (1 + g), pl.ds(peer(LAST[g][i]), 1), :]
                        place[k, 2 * g + src, i * cap : (i + 1) * cap, :] = jnp.where(hit, 1.0, 0.0).astype(BF16)
        for g in range(2):
            for src in range(2):
                rows_of = xnb if src else xall

                def tile(cols, g=g, src=src, rows_of=rows_of):
                    got = jnp.dot(place[k, 2 * g + src], rows_of[k, :, cols], preferred_element_type=F32).astype(BF16)
                    sbuf[src, :, :, cols] = got.reshape(4, cap, quarter)
                    drecv[k, source(0, g, src), :, cols] = sbuf[src, 0, :, cols]

                tiles(h, g, tile)
        for i in range(1, 4):
            for g in range(2):
                for src in range(2):
                    d_copy(s, h, g, src, i).start()

    def d_wait(k):
        for h in range(2):
            blocks(6, d_send.at[h], d_recv.at[k, h]).wait_recv()

    def send_back(s, h):
        k = chunk[s]
        for src in (1, 0):
            for i in range(1, 4):
                for g in range(2):
                    r_copy(s, h, g, src, i).start()
        for g in range(2):
            def tile(cols, g=g):
                for src in range(2):
                    rrecv[k, src, 0, :, cols] = drecv[k, source(0, g, src), :, cols]

            tiles(h, g, tile)

    def r_wait(s, h, src):
        k = chunk[s]
        blocks(3, r_send.at[s, h], r_recv.at[k, 2 * h + src]).wait_recv()

    def sum_neighbour(s, h):
        k = chunk[s]
        r_wait(s, h, 1)
        for g in range(2):
            def tile(cols, g=g):
                xnb[k, :, cols] = summed(k, g, 1, cols).astype(BF16)

            tiles(h, g, tile)
        for g in range(2):
            p_copy(s, h, g).start()

    def pass_on(s, h):
        k = chunk[s]
        r_wait(s, h, 0)
        pair(prcv, p_send.at[s, h], p_recv.at[k, h]).wait_recv()

        def own(g, cols):
            return summed(k, g, 0, cols) + prcv[k, :, cols].astype(F32)

        if s == 0:
            zr_wait(k1, h)
            zr_wait(k2, h)
            for g in range(2):
                def tile(cols, g=g):
                    total = own(g, cols) + xall[k, :, cols].astype(F32)
                    total = total + zret[k1, :, cols].astype(F32) + zret[k2, :, cols].astype(F32)
                    out_ref[:, cols] = total.astype(BF16)

                tiles(h, g, tile)
            return

        pair(xall, e_send.at[s, h], e_recv.at[k, h]).wait_send()

        @pl.when(inner == 1)
        def _():
            z_sent(s + 1, h)

        def plain():
            for g in range(2):
                def tile(cols, g=g):
                    xall[k, :, cols] = own(g, cols).astype(BF16)

                tiles(h, g, tile)

        if s == 1:
            plain()
            for g in range(2):
                zr_copy(k, h, g, s, z, k).start()
            return
        slot = z if s == 2 else k

        @pl.when(inner == 1)
        def _():
            zr_wait(slot, h)
            for g in range(2):
                def tile(cols, g=g):
                    xall[k, :, cols] = (own(g, cols) + zret[slot, :, cols].astype(F32)).astype(BF16)

                tiles(h, g, tile)
            for g in range(2):
                zr_copy(k, h, g, s, z, k).start()

        @pl.when(inner == 0)
        def _():
            plain()
            for g in range(2):
                zr_copy(k, h, g, s, k1 if s == 2 else k, k1).start()

    def slot_table():
        device = lax.broadcasted_iota(jnp.int32, (ndev, tok), 0)
        hit = None
        for j in range(ids_ref.shape[0]):
            here = lax.shift_right_logical(ids_ref[j : j + 1, :], 2) == device
            hit = here if hit is None else jnp.logical_or(hit, here)
        hit = jnp.where(hit, 1.0, 0.0)
        upto = lax.broadcasted_iota(jnp.int32, (tok, tok), 0) <= lax.broadcasted_iota(jnp.int32, (tok, tok), 1)
        upto = jnp.where(upto, 1.0, 0.0).astype(BF16)
        count = jnp.dot(hit.astype(BF16), upto, preferred_element_type=F32)
        slot = jnp.where(hit > 0.0, count - 1.0, -1.0).astype(jnp.int32)
        slot_ref[...] = slot.reshape(nz, nq, tok)

    def gate_table():
        row = lax.broadcasted_iota(jnp.int32, (ndev * 8, tok), 0)
        low = jnp.bitwise_and(row, 7)
        expert = jnp.where(low < 4, lax.shift_right_logical(row, 3) * 4 + low, -1)
        gate = jnp.zeros((ndev * 8, tok), F32)
        for j in range(ids_ref.shape[0]):
            gate = gate + jnp.where(ids_ref[j : j + 1, :] == expert, gates_ref[j : j + 1, :], 0.0)
        acc[0 : ndev * 8, 0:tok] = gate

        @pl.loop(0, ndev, unroll=4)
        def _(d):
            g = acc[pl.ds(pl.multiple_of(d * 8, 8), 8), 0:tok]
            hi = g.astype(BF16).astype(F32)
            mid = (g - hi).astype(BF16).astype(F32)
            low = g - hi - mid
            parts = jnp.concatenate([hi, mid, low, jnp.zeros_like(g)], axis=0).astype(BF16)
            slot = slot_ref[lax.div(d, nq), pl.ds(lax.rem(d, nq), 1), :]
            spot = lax.broadcasted_iota(jnp.int32, (128, tok), 0) == slot
            spot = jnp.where(spot, 1.0, 0.0).astype(BF16)
            got = lax.dot_general(parts, spot, (((1,), (1,)), ((), ())), preferred_element_type=F32)
            sgate_ref[d] = got[0:8] + got[8:16] + got[16:24]

    steps = {"e": swap_rows, "p": pick, "b": send_back, "n": sum_neighbour, "u": pass_on}

    def run(word):
        steps[word[0]](int(word[1]), int(word[2]))

    before, seen = {}, 0
    for word in ORDER:
        if word[0] == "c":
            seen += 1
        else:
            before.setdefault(seen, []).append(word)

    barrier = pltpu.get_barrier_semaphore()

    @pl.loop(1, ndev)
    def _(o):
        d = lax.rem(me + o, ndev)
        pl.semaphore_signal(barrier, inc=1, device_id=at(lax.div(d, nq), lax.rem(d, nq)), device_id_type=MESH)

    load_x = pltpu.make_async_copy(x_ref, xall.at[z], x_sem)
    load_x.start()
    for c in weight_copies(0, 0):
        c.start()
    slot_table()
    smap[z, 0] = slot_ref[z]
    load_x.wait()
    pl.semaphore_wait(barrier, ndev - 1)
    for h in range(2):
        for g in range(2):
            @pl.when(z > 0)
            def _():
                z_rows(z, z - 1, 0, h, g).start()

            @pl.when(z < nz - 1)
            def _():
                z_rows(z, z + 1, 1, h, g).start()

        swap_rows(0, h)
        for o in range(nz):
            for role in range(3):
                if h == 0 and (o or role):
                    slot_copy(o, role).start()
    gate_table()

    @pl.loop(1, ndev)
    def _(o):
        gate_copy(o).start()

    grecv[me] = sgate_ref[me]
    for word in before.get(0, ())[2:]:
        run(word)
    tables(grecv, ndev - 1, g_send, g_recv).wait_recv()

    def expert_step(i, _):
        s, e, slot = lax.div(i, 4), lax.rem(i, 4), lax.rem(i, 2)
        k = plane_of(s)

        for n in range(1, 16):
            if n in before:
                @pl.when(i == n)
                def _():
                    for word in before[n]:
                        run(word)

        down_copy(e).start()

        @pl.when(i < 15)
        def _():
            for c in weight_copies(lax.rem(i + 1, 4), 1 - slot):
                c.start()

        @pl.when(e == 0)
        def _():
            d_wait(k)
            by_slot = grecv[pl.ds(k * nq, nq)].reshape(nq * 8, 128).T
            for r in range(nq):
                for j in range(4):
                    one = by_slot[0:cap, r * 8 + j : r * 8 + j + 1]
                    gb[j, r * cap : (r + 1) * cap, :] = jnp.broadcast_to(one, (cap, 128))

        for c in weight_copies(e, slot):
            c.wait()

        @pl.loop(0, ff // ft, unroll=3)
        def _(n):
            cols = pl.ds(pl.multiple_of(n * ft, ft), ft)
            xin = drecv[k].reshape(rows, hid)
            a = jnp.dot(xin, wb1[slot, :, cols], preferred_element_type=F32)
            b = jnp.dot(xin, wb3[slot, :, cols], preferred_element_type=F32)
            hbuf[:, cols] = (a * jax.nn.sigmoid(a) * b).astype(BF16)

        down_copy(e).wait()

        @pl.loop(0, hid // ot, unroll=8)
        def _(n):
            cols = pl.ds(pl.multiple_of(n * ot, ot), ot)
            o = jnp.dot(hbuf[...], wb2[:, cols], preferred_element_type=F32)
            g = jnp.concatenate([gb[e]] * (ot // 128), axis=1)
            term = jnp.where(g > 0.0, o * g, 0.0)
            acc[:, cols] = jnp.where(e == 0, 0.0, acc[:, cols]) + term

        @pl.when(e == 3)
        def _():
            @pl.loop(0, hid // nt)
            def _(n):
                cols = pl.ds(pl.multiple_of(n * nt, nt), nt)
                drecv[k, :, :, cols] = acc[:, cols].astype(BF16).reshape(nq, cap, nt)

        return 0

    lax.fori_loop(0, 16, expert_step, 0)
    for word in before.get(16, ()):
        run(word)

    for h in range(2):
        @pl.when(z > 0)
        def _():
            z_sent(0, h)

        @pl.when(z < nz - 1)
        def _():
            z_sent(1, h)

        pair(xall, e_send.at[0, h], e_recv.at[0, h]).wait_send()
        for s in range(4):
            pair(xnb, p_send.at[s, h], p_recv.at[0, h]).wait_send()
            if s:
                pair(xall, zr_send.at[s, h], zr_recv.at[0, h]).wait_send()
            if s == 3:
                blocks(6, d_send.at[h], d_recv.at[0, h]).wait_send()
            blocks(6, r_send.at[s, h], r_recv.at[0, h]).wait_send()
    tables(sgate_ref, ndev - 1, g_send, g_recv).wait_send()
    tables(sgate_ref, 2 * (3 * nz - 1), sm_send, sm_recv.at[0]).wait_send()


def moe_call(dims, x, ids, gates, w1, w3, w2, capacity):
    nz, ny, nx = dims
    nq = ny * nx
    ndev = nz * nq
    tok, hid = x.shape
    ff = w1.shape[2]
    dma = pltpu.SemaphoreType.DMA
    vmem = pl.BlockSpec(memory_space=pltpu.VMEM)
    hbm = pl.BlockSpec(memory_space=pl.ANY)
    return pl.pallas_call(
        functools.partial(moe_kernel, dims),
        out_shape=jax.ShapeDtypeStruct((tok, hid), BF16),
        in_specs=[hbm, vmem, vmem, hbm, hbm, hbm],
        out_specs=vmem,
        scratch_shapes=[
            pltpu.VMEM((nz, nq, tok), jnp.int32),
            pltpu.VMEM((ndev, 8, 128), F32),
            pltpu.VMEM((nz, tok, hid), BF16),
            pltpu.VMEM((nz, tok, hid), BF16),
            pltpu.VMEM((nz, 3, nq, tok), jnp.int32),
            pltpu.VMEM((ndev, 8, 128), F32),
            pltpu.VMEM((nz, 4, 4 * capacity, tok), BF16),
            pltpu.VMEM((2, 4, capacity, hid), BF16),
            pltpu.VMEM((nz, nq, capacity, hid), BF16),
            pltpu.VMEM((nz, 2, 4, capacity, hid), BF16),
            pltpu.VMEM((nz, tok, hid), BF16),
            pltpu.VMEM((nz, tok, hid), BF16),
            pltpu.VMEM((nq * capacity, hid), F32),
            pltpu.VMEM((nq * capacity, ff), BF16),
            pltpu.VMEM((4, nq * capacity, 128), F32),
            pltpu.VMEM((2, hid, ff), BF16),
            pltpu.VMEM((2, hid, ff), BF16),
            pltpu.VMEM((ff, hid), BF16),
            dma,
            dma((2, 3)),
            dma((5, 2)),
            dma((nz, 2)),
            dma,
            dma((nz,)),
            dma,
            dma,
            dma((nz, 2)),
            dma((nz, 2)),
            dma((2,)),
            dma((nz, 2)),
            dma((nz, 2)),
            dma((nz, 4)),
            dma((nz, 2)),
            dma((nz, 2)),
            dma((nz, 2)),
            dma((nz, 2)),
        ],
        compiler_params=pltpu.CompilerParams(collective_id=0, has_side_effects=True, vmem_limit_bytes=67 * 1000 * 1000),
    )(x, ids, gates, w1, w3, w2)


def solution(mesh):
    ep_axes = tuple(mesh.axis_names)
    dims = tuple(mesh.shape[axis_name] for axis_name in ep_axes)
    num_devices = math.prod(dims)
    row_spec = P(ep_axes, None)
    w_spec = P(ep_axes, None, None)

    def local_layer(tokens, expert_ids, gate_weights, w_gate, w_up, w_down):
        tok_dev = tokens.shape[0]
        top_k = expert_ids.shape[1]
        capacity = tok_dev * top_k // num_devices
        return moe_call(dims, tokens, expert_ids.T, gate_weights.T, w_gate, w_up, w_down, capacity)

    return jax.shard_map(local_layer, mesh=mesh, in_specs=(row_spec, row_spec, row_spec, w_spec, w_spec, w_spec), out_specs=row_spec, check_vma=False)
```
